256 devices in a mesh: grp: 4 (over y), cp: 64 (over x, z, core).
Axes of the slice: x: 4, y: 4, z: 8, core: 2. Of those that a mesh axis runs over, the one named last changes fastest.
Arguments:
- queries: bfloat16 [131072, 2048], P(('grp', 'cp')), parts along dimension 0, may hold values from -6 to 6
- keys: bfloat16 [131072, 1024], P(('grp', 'cp')), parts along dimension 0, may hold values from -8 to 8
- values: bfloat16 [131072, 1024], P(('grp', 'cp')), parts along dimension 0, may hold values from -6 to 6
- doc_lengths: int32 [1024], P('grp'), parts along dimension 0, may hold values from 1 to 1024, 32768 in all
Outputs:
- attended: bfloat16 [131072, 2048], P(('grp', 'cp')), parts along dimension 0
The draws below stay inside these ranges and needn't reach their ends.
There are 4 independent parts, one for each index of `grp`. The reference program is written for one: setup_inputs(seed, part) draws one part's arguments, and reference() takes and returns one part's arrays. A program takes and returns all parts, laid end to end along the dimension named above; each array names one. Nothing has to cross between parts.
Inputs may be any that keep to these rules, and one draw needn't show every extreme that they name: doc_lengths sums to 32768, and its largest entry is exactly 1024.
All inputs are finite; a program needn't handle non-finite values.
Results may differ from the reference program's by a relative error of at most 0.0031.
Values may be sent and summed in bfloat16 or wider, within the bound.
No kernel may reach another device: no remote copies, remote signals or barrier semaphores. Data moves between devices by JAX's collectives and lax.ppermute only.
A program may use at most 64 MiB of HBM per device.

```python
import math
import jax
import jax.numpy as jnp
import numpy as np
from jax import lax

HQ = 16
HK = 8
DH = 128
TOK_DEV = 512
REACH = 2
TOKENS = 32768
MAXDOC = 1024
DOCS = 256


def draw_queries(key, part):
    drawn = jnp.clip(jax.random.normal(jax.random.fold_in(key, 11), (TOKENS, HQ * DH), jnp.float32), -6.0, 6.0)
    return drawn.astype(jnp.bfloat16)


def draw_keys(key, part):
    drawn = jnp.clip(jax.random.normal(jax.random.fold_in(key, 22), (TOKENS, HK * DH), jnp.float32), -6.0, 6.0)
    return drawn.astype(jnp.bfloat16)


def shard_levels(rng, extent, shards, low, largest):
    factor_of, own = 1.0, jax.random.fold_in(rng, 6)
    for dim, blocks in shards:
        draws = jnp.exp(jax.random.uniform(jax.random.fold_in(own, dim), (blocks,), jnp.float32, low / len(shards), largest / len(shards)))
        factor_of = factor_of * jnp.repeat(draws, extent[dim] // blocks).reshape([-1 if axis == dim else 1 for axis in range(len(extent))])
    return factor_of


def profile(count, total, bound, skew):
    weights = [(1 << 20) // math.isqrt(standing ** skew) + 1 for standing in range(2, count + 1)]
    surplus, given = total - bound - (count - 1), [1] * (count - 1)
    while surplus > 0:
        movable = [i for i in range(count - 1) if given[i] < bound]
        mass, remaining = sum([weights[i] for i in movable]), surplus
        for i in movable:
            extra = min(bound - given[i], max(1, remaining * weights[i] // mass), surplus)
            given[i] = given[i] + extra
            surplus = surplus - extra
    return np.array([bound] + given)


def ragged_sizes(key, number_of, total, most, skew):
    if number_of == 2:
        one = jax.random.randint(key, (), max(1, total - most), min(most, total - 1) + 1)
        return jnp.stack([one, total - one])
    lengths = jnp.asarray(profile(number_of, total, most, skew), jnp.int32)
    couples = (number_of - 1) // 2
    source_of, taker = lengths[1:1 + 2 * couples:2], lengths[2:2 + 2 * couples:2]
    room = jnp.minimum(source_of - 1, most - taker)
    passed = jax.random.randint(jax.random.fold_in(key, 1), (couples,), 0, 1 << 20) % (room + 1)
    lengths = lengths.at[1:1 + 2 * couples:2].set(source_of - passed).at[2:2 + 2 * couples:2].set(taker + passed)
    return lengths[jax.random.permutation(jax.random.fold_in(key, 2), number_of)]


def noise(rng, dims, spread, limit, shards=(), held_as=jnp.bfloat16):
    loudness = shard_levels(rng, dims, shards, -0.22, 0.18) if shards else 1.0
    array = jax.random.normal(rng, dims, jnp.float32) * spread * loudness
    return jnp.minimum(jnp.maximum(array, -limit), limit).astype(held_as)


def setup_inputs(seed: int = 0, part: int = 0) -> dict:
    arg_keys = jax.random.split(jax.random.key(seed), 5)
    part_splits = jax.random.split(jax.random.fold_in(arg_keys[4], part), 5)
    queries = draw_queries(jax.random.fold_in(jax.random.fold_in(arg_keys[4], part), 71), part)
    keys = draw_keys(jax.random.fold_in(jax.random.fold_in(arg_keys[4], part), 71), part)
    values = noise(part_splits[2], (TOKENS, HK * DH), 1.0, 6.0, ((0, 64),))
    doc_lengths = ragged_sizes(part_splits[3], DOCS, TOKENS, MAXDOC, 2).astype(jnp.int32)
    return {"queries": queries, "keys": keys, "values": values, "doc_lengths": doc_lengths}


query_scale = 144.0 ** -0.5


def doc_index(positions, doc_ends):
    return jnp.sum((positions[:, None] >= doc_ends[None, :]).astype(jnp.int32), axis=1).astype(jnp.int32)


def attend(query_rows, key_rows, value_rows, visible):
    tok_rows = query_rows.shape[0]
    key_count = key_rows.shape[0]
    groups = HQ // HK
    query_heads = query_rows.astype(jnp.float32).reshape(tok_rows, HK, groups, DH)
    key_heads = key_rows.astype(jnp.float32).reshape(key_count, HK, DH)
    value_heads = value_rows.astype(jnp.float32).reshape(key_count, HK, DH)
    scores = jnp.einsum("tkgd,wkd->kgtw", query_heads, key_heads) * query_scale
    scores = jnp.where(visible[None, None], scores, -jnp.inf)
    highest = jnp.max(scores, axis=-1, keepdims=True)
    weights = jnp.exp(scores - highest)
    totals = jnp.sum(weights, axis=-1)
    rounded = lax.optimization_barrier(weights.astype(jnp.bfloat16))
    mixed = jnp.einsum("kgtw,wkd->tkgd", rounded.astype(jnp.float32), value_heads)
    mixed = mixed / jnp.transpose(totals, (2, 0, 1))[..., None]
    return mixed.reshape(tok_rows, HQ * DH).astype(jnp.bfloat16)


def reference(queries, keys, values, doc_lengths):
    doc_ends = jnp.cumsum(doc_lengths).astype(jnp.int32)
    margin = REACH * TOK_DEV
    window = (REACH + 1) * TOK_DEV
    pad_keys = jnp.concatenate([jnp.zeros((margin, HK * DH), keys.dtype), keys], axis=0)
    pad_values = jnp.concatenate([jnp.zeros((margin, HK * DH), values.dtype), values], axis=0)

    def one_block(index):
        begin_row = (index * TOK_DEV).astype(jnp.int32)
        query_pos = begin_row + jnp.arange(TOK_DEV, dtype=jnp.int32)
        key_pos = begin_row - margin + jnp.arange(window, dtype=jnp.int32)
        same_doc = doc_index(query_pos, doc_ends)[:, None] == doc_index(key_pos, doc_ends)[None, :]
        visible = same_doc & (key_pos[None, :] <= query_pos[:, None]) & (key_pos[None, :] >= 0)
        query_rows = lax.dynamic_slice_in_dim(queries, begin_row, TOK_DEV, 0)
        key_rows = lax.dynamic_slice_in_dim(pad_keys, begin_row, window, 0)
        value_rows = lax.dynamic_slice_in_dim(pad_values, begin_row, window, 0)
        return attend(query_rows, key_rows, value_rows, visible)

    blocks = lax.map(one_block, jnp.arange(TOKENS // TOK_DEV, dtype=jnp.int32))
    return blocks.reshape(TOKENS, HQ * DH)
```

```python
import functools
import math

import jax
import jax.numpy as jnp
from jax import lax
from jax.experimental import pallas as pl
from jax.experimental.pallas import tpu as pltpu
from jax.sharding import PartitionSpec as P


HQ = 16
HK = 8
DH = 128
GROUPS = HQ // HK
WIDTH = GROUPS * DH
BQ = 128
HIDDEN = -1e30
RATE = math.log2(math.e) * 144.0 ** -0.5
START_LANE = 2 * HQ
VMEM = 24 << 20
INTERPRET = False


def document_ends(lengths):
    docs = lengths.shape[1]
    sub = lax.broadcasted_iota(jnp.int32, (docs, docs), 0)
    lane = lax.broadcasted_iota(jnp.int32, (docs, docs), 1)
    rows = jnp.broadcast_to(lengths.astype(jnp.float32), (docs, docs))
    column = jnp.sum(jnp.where(sub == lane, rows, 0.0), axis=1, keepdims=True)
    return jnp.sum(jnp.where(sub <= lane, column, 0.0), axis=0, keepdims=True)


def lane_column(table, lane):
    return table[:, lane : lane + 1]


def head_pair(ref, head):
    both = ref[:, head * WIDTH : (head + 1) * WIDTH]
    return jnp.concatenate([both[:, :DH], both[:, DH:]], axis=0)


def block_attention(queries, keys, values, bias, highest=None):
    rows = bias.shape[0]
    scores = lax.dot_general(queries, keys, (((1,), (1,)), ((), ())), preferred_element_type=jnp.float32)
    scores = scores.reshape(GROUPS, rows, -1) + bias[None]
    top = jnp.max(scores, axis=-1, keepdims=True)
    if highest is not None:
        top = jnp.maximum(top, highest)
    weights = jnp.exp2((scores - top) * RATE)
    totals = jnp.sum(weights, axis=-1, keepdims=True)
    rounded = weights.astype(jnp.bfloat16).reshape(GROUPS * rows, -1)
    mixed = lax.dot_general(rounded, values, (((1,), (0,)), ((), ())), preferred_element_type=jnp.float32)
    return mixed.reshape(GROUPS, rows, DH), top, totals


def own_kernel(first_ref, len_ref, q_ref, k_ref, v_ref, acc_ref, state_ref, ends_ref):
    block = pl.program_id(0)

    @pl.when(block == 0)
    def _():
        ends_ref[...] = document_ends(len_ref[...])

    ends = ends_ref[...]
    keys = k_ref.shape[0]
    first = first_ref[0].astype(jnp.float32)
    at = (block * BQ).astype(jnp.float32)
    row = lax.broadcasted_iota(jnp.int32, (BQ, 1), 0).astype(jnp.float32) + at
    start = jnp.max(jnp.where(ends <= row + first, ends, 0.0), axis=1, keepdims=True)
    col = lax.broadcasted_iota(jnp.int32, (BQ, keys), 1).astype(jnp.float32)
    bias = jnp.where((col >= start - first) & (col <= row), 0.0, HIDDEN)
    lane = lax.broadcasted_iota(jnp.int32, (BQ, 128), 1)
    state = jnp.broadcast_to(start, (BQ, 128))
    for head in range(HK):
        mixed, top, totals = block_attention(
            head_pair(q_ref, head), k_ref[:, head * DH : (head + 1) * DH], v_ref[:, head * DH : (head + 1) * DH], bias
        )
        for g in range(GROUPS):
            h = head * GROUPS + g
            acc_ref[:, h * DH : (h + 1) * DH] = mixed[g]
            state = jnp.where(lane == h, top[g], state)
            state = jnp.where(lane == HQ + h, totals[g], state)
    state_ref[...] = state


def more_kernel(last, base_ref, q_ref, k_ref, v_ref, acc_ref, state_ref, out_ref, *out_state):
    keys = k_ref.shape[0]
    base = base_ref[0].astype(jnp.float32)
    state = state_ref[...]
    start = lane_column(state, START_LANE)
    needed = jnp.min(start) < base + keys

    @pl.when(jnp.logical_not(needed))
    def _():
        for h in range(HQ):
            part = acc_ref[:, h * DH : (h + 1) * DH]
            if last:
                part = (part * (1.0 / lane_column(state, HQ + h))).astype(out_ref.dtype)
            out_ref[:, h * DH : (h + 1) * DH] = part
        if not last:
            out_state[0][...] = state

    @pl.when(needed)
    def _():
        col = lax.broadcasted_iota(jnp.int32, (BQ, keys), 1).astype(jnp.float32)
        bias = jnp.where(col >= start - base, 0.0, HIDDEN)
        lane = lax.broadcasted_iota(jnp.int32, (BQ, 128), 1)
        new = state
        for head in range(HK):
            heads = [head * GROUPS + g for g in range(GROUPS)]
            before = jnp.stack([lane_column(state, h) for h in heads])
            mixed, top, totals = block_attention(
                head_pair(q_ref, head), k_ref[:, head * DH : (head + 1) * DH], v_ref[:, head * DH : (head + 1) * DH], bias, before
            )
            keep = jnp.exp2((before - top) * RATE)
            for g, h in enumerate(heads):
                total = totals[g] + keep[g] * lane_column(state, HQ + h)
                part = mixed[g] + keep[g] * acc_ref[:, h * DH : (h + 1) * DH]
                if last:
                    part = (part * (1.0 / total)).astype(out_ref.dtype)
                else:
                    new = jnp.where(lane == h, top[g], new)
                    new = jnp.where(lane == HQ + h, total, new)
                out_ref[:, h * DH : (h + 1) * DH] = part
        if not last:
            out_state[0][...] = new


def whole():
    return pl.BlockSpec(memory_space=pltpu.VMEM)


def rows_of(width):
    return pl.BlockSpec((BQ, width), lambda i: (i, 0))


SMEM = pl.BlockSpec(memory_space=pltpu.SMEM)


def cost(rows, keys):
    flops = 4 * rows * keys * HQ * DH
    return pl.CostEstimate(flops=flops, bytes_accessed=rows * HQ * DH * 8, transcendentals=rows * keys * HQ)


def own_stage(first, lengths, queries, keys, values):
    rows = queries.shape[0]
    return pl.pallas_call(
        own_kernel,
        grid=(rows // BQ,),
        in_specs=[SMEM, whole(), rows_of(HQ * DH), whole(), whole()],
        out_specs=[rows_of(HQ * DH), rows_of(128)],
        out_shape=[jax.ShapeDtypeStruct((rows, HQ * DH), jnp.float32), jax.ShapeDtypeStruct((rows, 128), jnp.float32)],
        scratch_shapes=[pltpu.VMEM(lengths.shape, jnp.float32)],
        cost_estimate=cost(rows, keys.shape[0]),
        compiler_params=pltpu.CompilerParams(vmem_limit_bytes=VMEM),
        name="own_shard",
        interpret=INTERPRET,
    )(first, lengths, queries, keys, values)


def more_stage(base, queries, keys, values, acc, state, last):
    rows = queries.shape[0]
    out_specs = [rows_of(HQ * DH)] + ([] if last else [rows_of(128)])
    out_shape = [jax.ShapeDtypeStruct((rows, HQ * DH), jnp.bfloat16 if last else jnp.float32)]
    if not last:
        out_shape.append(jax.ShapeDtypeStruct((rows, 128), jnp.float32))
    return pl.pallas_call(
        functools.partial(more_kernel, last),
        grid=(rows // BQ,),
        in_specs=[SMEM, rows_of(HQ * DH), whole(), whole(), rows_of(HQ * DH), rows_of(128)],
        out_specs=out_specs,
        out_shape=out_shape,
        cost_estimate=cost(rows, keys.shape[0]),
        compiler_params=pltpu.CompilerParams(vmem_limit_bytes=VMEM),
        name="last_shard" if last else "next_shard",
        interpret=INTERPRET,
    )(base, queries, keys, values, acc, state)


def on_device(queries, keys, values, doc_lengths):
    rows = queries.shape[0]
    count = lax.axis_size("cp")
    first = lax.axis_index("cp").astype(jnp.int32) * rows
    onward = [(i, i + 1) for i in range(count - 1)]
    one_k = lax.ppermute(keys, "cp", onward)
    one_v = lax.ppermute(values, "cp", onward)
    two_k = lax.ppermute(one_k, "cp", onward)
    two_v = lax.ppermute(one_v, "cp", onward)
    lengths = doc_lengths.reshape(1, -1)
    acc, state = own_stage(first.reshape(1), lengths, queries, keys, values)
    acc, state = more_stage((first - rows).reshape(1), queries, one_k, one_v, acc, state, False)
    (out,) = more_stage((first - 2 * rows).reshape(1), queries, two_k, two_v, acc, state, True)
    return out


def solution(mesh):
    return jax.shard_map(
        on_device,
        mesh=mesh,
        in_specs=(P(("grp", "cp"), None), P(("grp", "cp"), None), P(("grp", "cp"), None), P("grp")),
        out_specs=P(("grp", "cp"), None),
        check_vma=False,
    )
```

```python
import math

import jax
import jax.numpy as jnp
from jax import lax
from jax.experimental import pallas as pl
from jax.experimental.pallas import tpu as pltpu
from jax.sharding import PartitionSpec as P


HQ = 16
HK = 8
DH = 128
GROUPS = HQ // HK
WIDTH = GROUPS * DH
KV = HK * DH
BQ = 128
HIDDEN = -1e30
RATE = math.log2(math.e) * 144.0 ** -0.5
START = 2 * HQ
PARTS = 3
VMEM = 24 << 20
INTERPRET = False

SLOT = 256


def document_ends(lengths):
    docs = lengths.shape[1]
    sub = lax.broadcasted_iota(jnp.int32, (docs, docs), 0)
    lane = lax.broadcasted_iota(jnp.int32, (docs, docs), 1)
    rows = jnp.broadcast_to(lengths.astype(jnp.float32), (docs, docs))
    column = jnp.sum(jnp.where(sub == lane, rows, 0.0), axis=1, keepdims=True)
    return jnp.sum(jnp.where(sub <= lane, column, 0.0), axis=0, keepdims=True)


def float_iota(shape, axis):
    return lax.broadcasted_iota(jnp.int32, shape, axis).astype(jnp.float32)


def attend(pair, keys, values, bias, before, emit):
    rows = bias.shape[0]

    def score(head):
        return lax.dot_general(pair(head), keys(head), (((1,), (1,)), ((), ())), preferred_element_type=jnp.float32)

    ahead = score(0)
    for head in range(HK):
        scores = ahead
        if head + 1 < HK:
            ahead = score(head + 1)
        scores = scores.reshape(GROUPS, rows, -1) + bias[None]
        top = jnp.max(scores, axis=-1, keepdims=True)
        if before is not None:
            top = jnp.maximum(top, before(head))
        weights = jnp.exp2((scores - top) * RATE)
        rounded = weights.astype(jnp.bfloat16).reshape(GROUPS * rows, -1)
        value = values(head)
        value = jnp.concatenate([value, jnp.ones_like(value)], axis=1)
        mixed = lax.dot_general(rounded, value, (((1,), (0,)), ((), ())), preferred_element_type=jnp.float32)
        mixed = mixed.reshape(GROUPS, rows, 2 * DH)
        for g in range(GROUPS):
            emit(head, g, mixed[g, :, :DH], mixed[g, :, DH:], top[g])


def heads_of(ref, rows=slice(None), at=0):
    return lambda head: ref[rows, at + head * DH : at + (head + 1) * DH]


def pairs_of(ref, rows=slice(None)):
    def pair(head):
        both = ref[rows, head * WIDTH : (head + 1) * WIDTH]
        return jnp.concatenate([both[:, :DH], both[:, DH:]], axis=0)

    return pair


def own_kernel(first_ref, len_ref, q_ref, k_ref, v_ref, acc_ref, state_ref, ends_ref):
    block = pl.program_id(0)

    @pl.when(block == 0)
    def _():
        ends_ref[...] = document_ends(len_ref[...])

    ends = ends_ref[...]
    keys = k_ref.shape[0]
    first = first_ref[0].astype(jnp.float32)
    row = float_iota((BQ, 1), 0) + (block * BQ).astype(jnp.float32)
    start = jnp.max(jnp.where(ends <= row + first, ends, 0.0), axis=1, keepdims=True)
    col = float_iota((BQ, keys), 1)
    bias = jnp.where((col >= start - first) & (col <= row), 0.0, HIDDEN)
    lane = lax.broadcasted_iota(jnp.int32, (BQ, 128), 1)
    state = [jnp.broadcast_to(start, (BQ, 128))]

    def emit(head, g, mixed, total, top):
        h = head * GROUPS + g
        acc_ref[:, h * DH : (h + 1) * DH] = mixed
        state[0] = jnp.where(lane == HQ + h, total, jnp.where(lane == h, top, state[0]))

    attend(pairs_of(q_ref), heads_of(k_ref), heads_of(v_ref), bias, None, emit)
    state_ref[...] = state[0]


def back_kernel(first_ref, len_ref, q_ref, k_ref, v_ref, slot_ref):
    first = first_ref[0]
    here = first.astype(jnp.float32)
    keys = k_ref.shape[0]
    block = pl.program_id(0)

    @pl.when((first // keys) % 2 == 0)
    def _():
        ends = document_ends(len_ref[...])
        edge = here + 2 * keys
        start = jnp.max(jnp.where(ends <= edge, ends, 0.0))
        right = jnp.min(jnp.where(ends > edge, ends, edge + edge)) - edge
        by_keys = here + keys - start <= SLOT

        @pl.when(by_keys)
        def _():
            rows = pl.ds(keys - SLOT + block * BQ, BQ)
            slot_ref[:, :KV] = k_ref[rows, :]
            slot_ref[:, KV : 2 * KV] = v_ref[rows, :]
            slot_ref[:, 2 * KV :] = jnp.zeros((BQ, 128), jnp.bfloat16)

        @pl.when(jnp.logical_not(by_keys))
        def _():
            row = float_iota((BQ, 1), 0) + (block * BQ).astype(jnp.float32)
            col = float_iota((BQ, keys), 1)
            bias = jnp.where((col >= start - here) & (row < right), 0.0, HIDDEN)
            lane = lax.broadcasted_iota(jnp.int32, (BQ, 128), 1)
            level = [jnp.zeros((BQ, 128), jnp.float32)]

            def emit(head, g, mixed, total, top):
                h = head * GROUPS + g
                slot_ref[:, h * DH : (h + 1) * DH] = (mixed * (1.0 / total)).astype(jnp.bfloat16)
                level[0] = jnp.where(lane % HQ == h, top * RATE + jnp.log2(total), level[0])

            attend(pairs_of(q_ref), heads_of(k_ref), heads_of(v_ref), bias, None, emit)
            rest = level[0]
            tail = jnp.zeros((BQ, 128), jnp.float32)
            for part in range(PARTS):
                piece = rest.astype(jnp.bfloat16).astype(jnp.float32)
                tail = jnp.where(lane // HQ == part, piece, tail)
                rest = rest - piece
            slot_ref[:, 2 * KV :] = tail.astype(jnp.bfloat16)


def column(state, lane):
    return state[:, lane : lane + 1]


def old_tops(state):
    return lambda head: jnp.stack([column(state, head * GROUPS + g) for g in range(GROUPS)])


def next_kernel(first_ref, q_ref, k_ref, v_ref, acc_ref, state_ref, out_ref, new_acc_ref, new_state_ref):
    keys = k_ref.shape[0]
    first = first_ref[0].astype(jnp.float32)
    base = first - keys
    state = state_ref[...]
    start = column(state, START)
    lowest = jnp.min(start)

    @pl.when(lowest >= first)
    def _():
        for h in range(HQ):
            cols = slice(h * DH, (h + 1) * DH)
            out_ref[:, cols] = (acc_ref[:, cols] * (1.0 / column(state, HQ + h))).astype(out_ref.dtype)
        new_state_ref[...] = state

    @pl.when(lowest < first)
    def _():
        bias = jnp.where(float_iota((BQ, keys), 1) >= start - base, 0.0, HIDDEN)
        lane = lax.broadcasted_iota(jnp.int32, (BQ, 128), 1)
        new = [state]

        def emit(head, g, mixed, total, top):
            h = head * GROUPS + g
            cols = slice(h * DH, (h + 1) * DH)
            keep = jnp.exp2((column(state, h) - top) * RATE)
            total = total + keep * column(state, HQ + h)
            mixed = mixed + keep * acc_ref[:, cols]
            new_acc_ref[:, cols] = mixed
            new[0] = jnp.where(lane == HQ + h, total, jnp.where(lane == h, top, new[0]))
            out_ref[:, cols] = (mixed * (1.0 / total)).astype(out_ref.dtype)

        attend(pairs_of(q_ref), heads_of(k_ref), heads_of(v_ref), bias, old_tops(state), emit)
        new_state_ref[...] = new[0]


def last_kernel(first_ref, q_ref, slot_ref, k_ref, v_ref, acc_ref, state_ref, prior_ref, out_ref, rows_ref, sem):
    keys = k_ref.shape[0]
    first = first_ref[0].astype(jnp.float32)
    odd = (first_ref[0] // keys) % 2 == 1
    base = first - keys
    blocks = q_ref.shape[0] // BQ
    by_keys = base - jnp.min(state_ref[:8, START : START + 1]) <= SLOT

    def reaches(block):
        return jnp.min(state_ref[pl.ds(block * BQ, 8), START : START + 1]) < base

    def copy(block):
        rows = pl.ds(pl.multiple_of(block * BQ, BQ), BQ)
        return pltpu.make_async_copy(rows_ref.at[rows, :], out_ref.at[rows, :], sem.at[block])

    def merge(block, get_keys, get_values, count, origin):
        rows = pl.ds(pl.multiple_of(block * BQ, BQ), BQ)
        state = state_ref[rows, :]
        start = column(state, START)
        bias = jnp.where(float_iota((BQ, count), 1) >= start - origin, 0.0, HIDDEN)

        def emit(head, g, mixed, total, top):
            h = head * GROUPS + g
            cols = slice(h * DH, (h + 1) * DH)
            keep = jnp.exp2((column(state, h) - top) * RATE)
            total = total + keep * column(state, HQ + h)
            mixed = mixed + keep * acc_ref[rows, cols]
            rows_ref[rows, cols] = (mixed * (1.0 / total)).astype(rows_ref.dtype)

        attend(pairs_of(q_ref, rows), get_keys, get_values, bias, old_tops(state), emit)

    def combine(block):
        rows = pl.ds(pl.multiple_of(block * BQ, BQ), BQ)
        state = state_ref[rows, :]
        tail = slot_ref[rows, 2 * KV :].astype(jnp.float32)
        for h in range(HQ):
            cols = slice(h * DH, (h + 1) * DH)
            there = sum(column(tail, part * HQ + h) for part in reversed(range(PARTS)))
            here = column(state, h) * RATE
            top = jnp.maximum(here, there)
            keep, take = jnp.exp2(here - top), jnp.exp2(there - top)
            scale = 1.0 / (keep * column(state, HQ + h) + take)
            mixed = acc_ref[rows, cols] * (keep * scale) + slot_ref[rows, cols].astype(jnp.float32) * (take * scale)
            rows_ref[rows, cols] = mixed.astype(rows_ref.dtype)

    @pl.loop(0, blocks)
    def _(block):
        needed = reaches(block)

        @pl.when(needed & odd)
        def _():
            merge(block, heads_of(k_ref), heads_of(v_ref), keys, base - keys)

        @pl.when(needed & jnp.logical_not(odd) & by_keys)
        def _():
            merge(block, heads_of(slot_ref), heads_of(slot_ref, at=KV), SLOT, base - SLOT)

        @pl.when(needed & jnp.logical_not(odd) & jnp.logical_not(by_keys) & (block * BQ < SLOT))
        def _():
            combine(block)

        @pl.when(needed)
        def _():
            copy(block).start()

    @pl.loop(0, blocks)
    def _(block):
        @pl.when(reaches(block))
        def _():
            copy(block).wait()


def rows_of(width):
    return pl.BlockSpec((BQ, width), lambda i: (i, 0))


SMEM = pl.BlockSpec(memory_space=pltpu.SMEM)
WHOLE = pl.BlockSpec(memory_space=pltpu.VMEM)
WIDE = HQ * DH


def cost(rows, keys):
    return pl.CostEstimate(
        flops=4 * rows * keys * WIDE, bytes_accessed=rows * WIDE * 8, transcendentals=rows * keys * HQ
    )


PARAMS = pltpu.CompilerParams(vmem_limit_bytes=VMEM)


def f32(*shape):
    return jax.ShapeDtypeStruct(shape, jnp.float32)


def bf16(*shape):
    return jax.ShapeDtypeStruct(shape, jnp.bfloat16)


def own_stage(first, lengths, queries, keys, values):
    rows = queries.shape[0]
    return pl.pallas_call(
        own_kernel,
        grid=(rows // BQ,),
        in_specs=[SMEM, WHOLE, rows_of(WIDE), WHOLE, WHOLE],
        out_specs=[rows_of(WIDE), rows_of(128)],
        out_shape=[f32(rows, WIDE), f32(rows, 128)],
        scratch_shapes=[pltpu.VMEM(lengths.shape, jnp.float32)],
        cost_estimate=cost(rows, keys.shape[0]),
        compiler_params=PARAMS,
        name="own_shard",
        interpret=INTERPRET,
    )(first, lengths, queries, keys, values)


def back_stage(first, lengths, queries, keys, values):
    return pl.pallas_call(
        back_kernel,
        grid=(SLOT // BQ,),
        in_specs=[SMEM, WHOLE, rows_of(WIDE), WHOLE, WHOLE],
        out_specs=rows_of(2 * KV + 128),
        out_shape=bf16(SLOT, 2 * KV + 128),
        cost_estimate=cost(SLOT, keys.shape[0]),
        compiler_params=PARAMS,
        name="back_shard",
        interpret=INTERPRET,
    )(first, lengths, queries, keys, values)


def next_stage(first, queries, keys, values, acc, state):
    rows = queries.shape[0]
    return pl.pallas_call(
        next_kernel,
        grid=(rows // BQ,),
        in_specs=[SMEM, rows_of(WIDE), WHOLE, WHOLE, rows_of(WIDE), rows_of(128)],
        out_specs=[rows_of(WIDE), rows_of(WIDE), rows_of(128)],
        out_shape=[bf16(rows, WIDE), f32(rows, WIDE), f32(rows, 128)],
        cost_estimate=cost(rows, keys.shape[0]),
        compiler_params=PARAMS,
        name="next_shard",
        interpret=INTERPRET,
    )(first, queries, keys, values, acc, state)


def last_stage(first, queries, slot, keys, values, acc, state, prior):
    rows = queries.shape[0]
    return pl.pallas_call(
        last_kernel,
        in_specs=[SMEM, WHOLE, WHOLE, WHOLE, WHOLE, WHOLE, WHOLE, pl.BlockSpec(memory_space=pl.ANY)],
        out_specs=pl.BlockSpec(memory_space=pl.ANY),
        out_shape=bf16(rows, WIDE),
        scratch_shapes=[pltpu.VMEM((rows, WIDE), jnp.bfloat16), pltpu.SemaphoreType.DMA((rows // BQ,))],
        input_output_aliases={7: 0},
        cost_estimate=cost(rows, SLOT),
        compiler_params=PARAMS,
        name="last_shard",
        interpret=INTERPRET,
    )(first, queries, slot, keys, values, acc, state, prior)


def on_device(queries, keys, values, doc_lengths):
    count = lax.axis_size("cp")
    first = (lax.axis_index("cp").astype(jnp.int32) * queries.shape[0]).reshape(1)
    lengths = doc_lengths.reshape(1, -1)
    evens = range(0, count, 2)

    def hop(array, pairs):
        return lax.ppermute(array, "cp", pairs)

    onward = [(i, i + 1) for i in range(count - 1)]
    one_k = hop(keys, onward)
    one_v = hop(values, onward)
    guests = hop(queries[:SLOT], [(i, i - 2) for i in evens if i])
    acc, state = own_stage(first, lengths, queries, keys, values)
    slot = back_stage(first, lengths, guests, keys, values)
    slot = hop(slot, [(i, i + 2) for i in evens if i + 2 < count])
    across = [(i, i + 1) for i in evens]
    two_k = hop(one_k, across)
    two_v = hop(one_v, across)
    out, acc, state_next = next_stage(first, queries, one_k, one_v, acc, state)
    out = last_stage(first, queries, slot, two_k, two_v, acc, state_next, out)
    return out


def solution(mesh):
    return jax.shard_map(
        on_device,
        mesh=mesh,
        in_specs=(P(("grp", "cp"), None), P(("grp", "cp"), None), P(("grp", "cp"), None), P("grp")),
        out_specs=P(("grp", "cp"), None),
        check_vma=False,
    )
```

```python
import math

import jax
import jax.numpy as jnp
from jax import lax
from jax.experimental import pallas as pl
from jax.experimental.pallas import tpu as pltpu
from jax.sharding import PartitionSpec as P


HQ = 16
HK = 8
DH = 128
GROUPS = HQ // HK
WIDTH = GROUPS * DH
KV = HK * DH
BQ = 128
HIDDEN = -1e30
RATE = math.log2(math.e) * 144.0 ** -0.5
START = 2 * HQ
PARTS = 3
VMEM = 24 << 20
INTERPRET = False

SLOT = 256


def document_ends(lengths):
    docs = lengths.shape[1]
    sub = lax.broadcasted_iota(jnp.int32, (docs, docs), 0)
    lane = lax.broadcasted_iota(jnp.int32, (docs, docs), 1)
    rows = jnp.broadcast_to(lengths.astype(jnp.float32), (docs, docs))
    column = jnp.sum(jnp.where(sub == lane, rows, 0.0), axis=1, keepdims=True)
    return jnp.sum(jnp.where(sub <= lane, column, 0.0), axis=0, keepdims=True)


def float_iota(shape, axis):
    return lax.broadcasted_iota(jnp.int32, shape, axis).astype(jnp.float32)


def attend(pair, keys, values, bias, emit):
    rows = bias.shape[0]

    def score(head):
        return lax.dot_general(pair(head), keys(head), (((1,), (1,)), ((), ())), preferred_element_type=jnp.float32)

    ahead = score(0)
    for head in range(HK):
        scores = ahead
        if head + 1 < HK:
            ahead = score(head + 1)
        scores = scores.reshape(GROUPS, rows, -1) + bias[None]
        top = jnp.max(scores, axis=-1, keepdims=True)
        weights = jnp.exp2((scores - top) * RATE)
        rounded = weights.astype(jnp.bfloat16).reshape(GROUPS * rows, -1)
        value = values(head)
        value = jnp.concatenate([value, jnp.ones_like(value)], axis=1)
        mixed = lax.dot_general(rounded, value, (((1,), (0,)), ((), ())), preferred_element_type=jnp.float32)
        mixed = mixed.reshape(GROUPS, rows, 2 * DH)
        for g in range(GROUPS):
            emit(head, g, mixed[g, :, :DH], mixed[g, :, DH:], top[g])


def heads_of(ref, rows=slice(None), at=0):
    return lambda head: ref[rows, at + head * DH : at + (head + 1) * DH]


def pairs_of(ref, rows=slice(None)):
    def pair(head):
        both = ref[rows, head * WIDTH : (head + 1) * WIDTH]
        return jnp.concatenate([both[:, :DH], both[:, DH:]], axis=0)

    return pair


def own_kernel(first_ref, len_ref, q_ref, k_ref, v_ref, acc_ref, state_ref, ends_ref):
    block = pl.program_id(0)

    @pl.when(block == 0)
    def _():
        ends_ref[...] = document_ends(len_ref[...])

    ends = ends_ref[...]
    keys = k_ref.shape[0]
    first = first_ref[0].astype(jnp.float32)
    row = float_iota((BQ, 1), 0) + (block * BQ).astype(jnp.float32)
    start = jnp.max(jnp.where(ends <= row + first, ends, 0.0), axis=1, keepdims=True)
    col = float_iota((BQ, keys), 1)
    bias = jnp.where((col >= start - first) & (col <= row), 0.0, HIDDEN)
    lane = lax.broadcasted_iota(jnp.int32, (BQ, 128), 1)
    state = [jnp.broadcast_to(start, (BQ, 128))]

    def emit(head, g, mixed, total, top):
        h = head * GROUPS + g
        acc_ref[:, h * DH : (h + 1) * DH] = mixed
        state[0] = jnp.where(lane == HQ + h, total, jnp.where(lane == h, top, state[0]))

    attend(pairs_of(q_ref), heads_of(k_ref), heads_of(v_ref), bias, emit)
    state_ref[...] = state[0]


def back_kernel(first_ref, len_ref, q_ref, k_ref, v_ref, slot_ref):
    first = first_ref[0]
    here = first.astype(jnp.float32)
    keys = k_ref.shape[0]
    block = pl.program_id(0)

    @pl.when((first // keys) % 2 == 0)
    def _():
        ends = document_ends(len_ref[...])
        edge = here + 2 * keys
        start = jnp.max(jnp.where(ends <= edge, ends, 0.0))
        right = jnp.min(jnp.where(ends > edge, ends, edge + edge)) - edge
        by_keys = here + keys - start <= SLOT

        @pl.when(by_keys)
        def _():
            rows = pl.ds(keys - SLOT + block * BQ, BQ)
            slot_ref[:, :KV] = k_ref[rows, :]
            slot_ref[:, KV : 2 * KV] = v_ref[rows, :]
            slot_ref[:, 2 * KV :] = jnp.zeros((BQ, 128), jnp.bfloat16)

        @pl.when(jnp.logical_not(by_keys))
        def _():
            row = float_iota((BQ, 1), 0) + (block * BQ).astype(jnp.float32)
            col = float_iota((BQ, keys), 1)
            bias = jnp.where((col >= start - here) & (row < right), 0.0, HIDDEN)
            lane = lax.broadcasted_iota(jnp.int32, (BQ, 128), 1)
            level = [jnp.zeros((BQ, 128), jnp.float32)]

            def emit(head, g, mixed, total, top):
                h = head * GROUPS + g
                slot_ref[:, h * DH : (h + 1) * DH] = (mixed * (1.0 / total)).astype(jnp.bfloat16)
                level[0] = jnp.where(lane % HQ == h, top * RATE + jnp.log2(total), level[0])

            attend(pairs_of(q_ref), heads_of(k_ref), heads_of(v_ref), bias, emit)
            rest = level[0]
            tail = jnp.zeros((BQ, 128), jnp.float32)
            for part in range(PARTS):
                piece = rest.astype(jnp.bfloat16).astype(jnp.float32)
                tail = jnp.where(lane // HQ == part, piece, tail)
                rest = rest - piece
            slot_ref[:, 2 * KV :] = tail.astype(jnp.bfloat16)


def column(state, lane):
    return state[:, lane : lane + 1]


def heads_lanes(state, group):
    return pltpu.roll(state, 128 - group * HQ, 1) if group else state


def collect(fresh_ref):
    rows = fresh_ref.shape[0]
    lane = lax.broadcasted_iota(jnp.int32, (rows, 128), 1)
    held = [jnp.zeros((rows, 128), jnp.float32)]

    def emit(head, g, mixed, total, top):
        h = head * GROUPS + g
        fresh_ref[:, h * DH : (h + 1) * DH] = mixed
        held[0] = jnp.where(lane == HQ + h, total, jnp.where(lane == h, top, held[0]))

    return emit, held


def joined(state, fresh, normalised):
    top = jnp.maximum(state, fresh)
    keep = jnp.exp2((state - top) * RATE)
    take = jnp.exp2((fresh - top) * RATE)
    before = keep * heads_lanes(state, 1)
    total = before + take * heads_lanes(fresh, 1)
    scale = 1.0 / total
    return (before if normalised else keep) * scale, take * scale, top, total


def next_kernel(
    first_ref, q_ref, k_ref, v_ref, acc_ref, state_ref, out_ref, new_acc_ref, new_state_ref, fresh_ref
):
    keys = k_ref.shape[0]
    first = first_ref[0].astype(jnp.float32)
    base = first - keys
    state = state_ref[...]
    start = column(state, START)
    lowest = jnp.min(start)

    @pl.when(lowest >= first)
    def _():
        scale = 1.0 / heads_lanes(state, 1)
        for h in range(HQ):
            cols = slice(h * DH, (h + 1) * DH)
            out_ref[:, cols] = (acc_ref[:, cols] * column(scale, h)).astype(out_ref.dtype)
        new_state_ref[...] = state

    @pl.when(lowest < first)
    def _():
        bias = jnp.where(float_iota((BQ, keys), 1) >= start - base, 0.0, HIDDEN)
        emit, held = collect(fresh_ref)
        attend(pairs_of(q_ref), heads_of(k_ref), heads_of(v_ref), bias, emit)
        keep, take, top, total = joined(state, held[0], False)
        lane = lax.broadcasted_iota(jnp.int32, (BQ, 128), 1)
        totals = pltpu.roll(total, HQ, 1)
        new_state_ref[...] = jnp.where(lane < HQ, top, jnp.where(lane < 2 * HQ, totals, state))
        for h in range(HQ):
            cols = slice(h * DH, (h + 1) * DH)
            mixed = acc_ref[:, cols] * column(keep, h) + fresh_ref[:, cols] * column(take, h)
            new_acc_ref[:, cols] = mixed
            out_ref[:, cols] = mixed.astype(out_ref.dtype)


def last_kernel(
    first_ref, q_ref, slot_ref, k_ref, v_ref, acc_ref, state_ref, prior_ref, out_ref, rows_ref, fresh_ref, sem
):
    keys = k_ref.shape[0]
    first = first_ref[0].astype(jnp.float32)
    odd = (first_ref[0] // keys) % 2 == 1
    even = jnp.logical_not(odd)
    base = first - keys
    blocks = q_ref.shape[0] // BQ
    by_keys = base - jnp.min(state_ref[:8, START : START + 1]) <= SLOT

    def earliest(block):
        return jnp.min(state_ref[pl.ds(block * BQ, 8), START : START + 1])

    def copy(block):
        rows = pl.ds(pl.multiple_of(block * BQ, BQ), BQ)
        return pltpu.make_async_copy(rows_ref.at[rows, :], out_ref.at[rows, :], sem.at[block])

    def write(rows, keep, take, added_ref, added_rows):
        for h in range(HQ):
            cols = slice(h * DH, (h + 1) * DH)
            mixed = acc_ref[rows, cols] * column(keep, h) + added_ref[added_rows, cols].astype(jnp.float32) * column(take, h)
            rows_ref[rows, cols] = mixed.astype(rows_ref.dtype)

    def merge(block, get_keys, get_values, count, origin):
        rows = pl.ds(pl.multiple_of(block * BQ, BQ), BQ)
        state = state_ref[rows, :]
        bias = jnp.where(float_iota((BQ, count), 1) >= column(state, START) - origin, 0.0, HIDDEN)
        emit, held = collect(fresh_ref)
        attend(pairs_of(q_ref, rows), get_keys, get_values, bias, emit)
        keep, take, _, _ = joined(state, held[0], True)
        write(rows, keep, take, fresh_ref, slice(None))

    def combine(block):
        rows = pl.ds(pl.multiple_of(block * BQ, BQ), BQ)
        state = state_ref[rows, :]
        parts = slot_ref[rows, 2 * KV :].astype(jnp.float32)
        there = sum(heads_lanes(parts, part) for part in reversed(range(PARTS)))
        here = state * RATE
        top = jnp.maximum(here, there)
        before = jnp.exp2(here - top) * heads_lanes(state, 1)
        take = jnp.exp2(there - top)
        scale = 1.0 / (before + take)
        write(rows, before * scale, take * scale, slot_ref, rows)

    @pl.loop(0, blocks)
    def _(block):
        start = earliest(block)
        needed = start < base
        far = start < base - SLOT

        @pl.when(odd & far)
        def _():
            merge(block, heads_of(k_ref), heads_of(v_ref), keys, base - keys)

        @pl.when(odd & needed & jnp.logical_not(far))
        def _():
            near = slice(keys - SLOT, keys)
            merge(block, heads_of(k_ref, near), heads_of(v_ref, near), SLOT, base - SLOT)

        @pl.when(even & needed & by_keys)
        def _():
            merge(block, heads_of(slot_ref), heads_of(slot_ref, at=KV), SLOT, base - SLOT)

        @pl.when(even & needed & jnp.logical_not(by_keys) & (block * BQ < SLOT))
        def _():
            combine(block)

        @pl.when(needed)
        def _():
            copy(block).start()

    @pl.loop(0, blocks)
    def _(block):
        @pl.when(earliest(block) < base)
        def _():
            copy(block).wait()


def rows_of(width):
    return pl.BlockSpec((BQ, width), lambda i: (i, 0))


SMEM = pl.BlockSpec(memory_space=pltpu.SMEM)
WHOLE = pl.BlockSpec(memory_space=pltpu.VMEM)
WIDE = HQ * DH


def cost(rows, keys):
    return pl.CostEstimate(
        flops=4 * rows * keys * WIDE, bytes_accessed=rows * WIDE * 8, transcendentals=rows * keys * HQ
    )


PARAMS = pltpu.CompilerParams(vmem_limit_bytes=VMEM)


def f32(*shape):
    return jax.ShapeDtypeStruct(shape, jnp.float32)


def bf16(*shape):
    return jax.ShapeDtypeStruct(shape, jnp.bfloat16)


def own_stage(first, lengths, queries, keys, values):
    rows = queries.shape[0]
    return pl.pallas_call(
        own_kernel,
        grid=(rows // BQ,),
        in_specs=[SMEM, WHOLE, rows_of(WIDE), WHOLE, WHOLE],
        out_specs=[rows_of(WIDE), rows_of(128)],
        out_shape=[f32(rows, WIDE), f32(rows, 128)],
        scratch_shapes=[pltpu.VMEM(lengths.shape, jnp.float32)],
        cost_estimate=cost(rows, keys.shape[0]),
        compiler_params=PARAMS,
        name="own_shard",
        interpret=INTERPRET,
    )(first, lengths, queries, keys, values)


def copy_kernel(in_ref, out_ref):
    out_ref[...] = in_ref[...]


def leading_rows(array, rows):
    block = pl.BlockSpec((rows, array.shape[1]), lambda i: (0, 0))
    return pl.pallas_call(
        copy_kernel,
        grid=(1,),
        in_specs=[block],
        out_specs=block,
        out_shape=jax.ShapeDtypeStruct((rows, array.shape[1]), array.dtype),
        compiler_params=PARAMS,
        name="leading_rows",
        interpret=INTERPRET,
    )(array)


def back_stage(first, lengths, queries, keys, values):
    return pl.pallas_call(
        back_kernel,
        grid=(SLOT // BQ,),
        in_specs=[SMEM, WHOLE, rows_of(WIDE), WHOLE, WHOLE],
        out_specs=rows_of(2 * KV + 128),
        out_shape=bf16(SLOT, 2 * KV + 128),
        cost_estimate=cost(SLOT, keys.shape[0]),
        compiler_params=PARAMS,
        name="back_shard",
        interpret=INTERPRET,
    )(first, lengths, queries, keys, values)


def next_stage(first, queries, keys, values, acc, state):
    rows = queries.shape[0]
    return pl.pallas_call(
        next_kernel,
        grid=(rows // BQ,),
        in_specs=[SMEM, rows_of(WIDE), WHOLE, WHOLE, rows_of(WIDE), rows_of(128)],
        out_specs=[rows_of(WIDE), rows_of(WIDE), rows_of(128)],
        out_shape=[bf16(rows, WIDE), f32(rows, WIDE), f32(rows, 128)],
        scratch_shapes=[pltpu.VMEM((BQ, WIDE), jnp.float32)],
        cost_estimate=cost(rows, keys.shape[0]),
        compiler_params=PARAMS,
        name="next_shard",
        interpret=INTERPRET,
    )(first, queries, keys, values, acc, state)


def last_stage(first, queries, slot, keys, values, acc, state, prior):
    rows = queries.shape[0]
    return pl.pallas_call(
        last_kernel,
        in_specs=[SMEM, WHOLE, WHOLE, WHOLE, WHOLE, WHOLE, WHOLE, pl.BlockSpec(memory_space=pl.ANY)],
        out_specs=pl.BlockSpec(memory_space=pl.ANY),
        out_shape=bf16(rows, WIDE),
        scratch_shapes=[
            pltpu.VMEM((rows, WIDE), jnp.bfloat16),
            pltpu.VMEM((BQ, WIDE), jnp.float32),
            pltpu.SemaphoreType.DMA((rows // BQ,)),
        ],
        input_output_aliases={7: 0},
        cost_estimate=cost(rows, SLOT),
        compiler_params=PARAMS,
        name="last_shard",
        interpret=INTERPRET,
    )(first, queries, slot, keys, values, acc, state, prior)


def on_device(queries, keys, values, doc_lengths):
    count = lax.axis_size("cp")
    first = (lax.axis_index("cp").astype(jnp.int32) * queries.shape[0]).reshape(1)
    lengths = doc_lengths.reshape(1, -1)
    evens = range(0, count, 2)

    def hop(array, pairs):
        return lax.ppermute(array, "cp", pairs)

    onward = [(i, i + 1) for i in range(count - 1)]
    one_k = hop(keys, onward)
    one_v = hop(values, onward)
    guests = hop(leading_rows(queries, SLOT), [(i, i - 2) for i in evens if i])
    acc, state = own_stage(first, lengths, queries, keys, values)
    slot = back_stage(first, lengths, guests, keys, values)
    slot = hop(slot, [(i, i + 2) for i in evens if i + 2 < count])
    across = [(i, i + 1) for i in evens]
    two_k = hop(one_k, across)
    two_v = hop(one_v, across)
    out, acc, state_next = next_stage(first, queries, one_k, one_v, acc, state)
    out = last_stage(first, queries, slot, two_k, two_v, acc, state_next, out)
    return out


def solution(mesh):
    return jax.shard_map(
        on_device,
        mesh=mesh,
        in_specs=(P(("grp", "cp"), None), P(("grp", "cp"), None), P(("grp", "cp"), None), P("grp")),
        out_specs=P(("grp", "cp"), None),
        check_vma=False,
    )
```

```python
import math

import jax
import jax.numpy as jnp
from jax import lax
from jax.experimental import pallas as pl
from jax.experimental.pallas import tpu as pltpu
from jax.sharding import PartitionSpec as P


HQ = 16
HK = 8
DH = 128
GROUPS = HQ // HK
WIDTH = GROUPS * DH
KV = HK * DH
BQ = 128
HIDDEN = -1e30
RATE = math.log2(math.e) * 144.0 ** -0.5
START = 2 * HQ
PARTS = 3
VMEM = 24 << 20
INTERPRET = False

SLOT = 256


def document_ends(lengths):
    docs = lengths.shape[1]
    sub = lax.broadcasted_iota(jnp.int32, (docs, docs), 0)
    lane = lax.broadcasted_iota(jnp.int32, (docs, docs), 1)
    rows = jnp.broadcast_to(lengths.astype(jnp.float32), (docs, docs))
    column = jnp.sum(jnp.where(sub == lane, rows, 0.0), axis=1, keepdims=True)
    return jnp.sum(jnp.where(sub <= lane, column, 0.0), axis=0, keepdims=True)


def float_iota(shape, axis):
    return lax.broadcasted_iota(jnp.int32, shape, axis).astype(jnp.float32)


def attend(pair, keys, values, bias, emit):
    rows = bias.shape[0]

    def score(head):
        return lax.dot_general(pair(head), keys(head), (((1,), (1,)), ((), ())), preferred_element_type=jnp.float32)

    ahead = score(0)
    for head in range(HK):
        scores = ahead
        if head + 1 < HK:
            ahead = score(head + 1)
        scores = scores.reshape(GROUPS, rows, -1) + bias[None]
        top = jnp.max(scores, axis=-1, keepdims=True)
        weights = jnp.exp2((scores - top) * RATE)
        rounded = weights.astype(jnp.bfloat16).reshape(GROUPS * rows, -1)
        value = values(head)
        value = jnp.concatenate([value, jnp.ones_like(value)], axis=1)
        mixed = lax.dot_general(rounded, value, (((1,), (0,)), ((), ())), preferred_element_type=jnp.float32)
        mixed = mixed.reshape(GROUPS, rows, 2 * DH)
        for g in range(GROUPS):
            emit(head, g, mixed[g, :, :DH], mixed[g, :, DH:], top[g])


def heads_of(ref, rows=slice(None), at=0):
    return lambda head: ref[rows, at + head * DH : at + (head + 1) * DH]


def pairs_of(ref, rows=slice(None)):
    def pair(head):
        both = ref[rows, head * WIDTH : (head + 1) * WIDTH]
        return jnp.concatenate([both[:, :DH], both[:, DH:]], axis=0)

    return pair


def in_parts(table):
    rest = jnp.where(lax.broadcasted_iota(jnp.int32, table.shape, 1) < HQ, table, 0.0)
    parts = jnp.zeros_like(table)
    for part in range(PARTS):
        piece = rest.astype(jnp.bfloat16).astype(jnp.float32)
        parts = parts + (pltpu.roll(piece, part * HQ, 1) if part else piece)
        rest = rest - piece
    return parts.astype(jnp.bfloat16)


def spreader():
    sub = lax.broadcasted_iota(jnp.int32, (128, HQ * DH), 0)
    lane = lax.broadcasted_iota(jnp.int32, (128, HQ * DH), 1)
    return jnp.where((sub < PARTS * HQ) & (sub % HQ == lane // DH), 1.0, 0.0).astype(jnp.bfloat16)


def mix(keep, kept, take, taken, spread_ref, write):
    rows = keep.shape[0]
    table = jnp.concatenate([in_parts(keep), in_parts(take)], axis=0)
    for head in range(HK):
        cols = slice(head * WIDTH, (head + 1) * WIDTH)
        factors = jnp.dot(table, spread_ref[:, cols], preferred_element_type=jnp.float32)
        write(cols, factors[:rows] * kept(cols) + factors[rows:] * taken(cols).astype(jnp.float32))


def own_kernel(first_ref, len_ref, q_ref, k_ref, v_ref, acc_ref, state_ref, ends_ref):
    block = pl.program_id(0)

    @pl.when(block == 0)
    def _():
        ends_ref[...] = document_ends(len_ref[...])

    ends = ends_ref[...]
    keys = k_ref.shape[0]
    first = first_ref[0].astype(jnp.float32)
    row = float_iota((BQ, 1), 0) + (block * BQ).astype(jnp.float32)
    start = jnp.max(jnp.where(ends <= row + first, ends, 0.0), axis=1, keepdims=True)
    col = float_iota((BQ, keys), 1)
    bias = jnp.where((col >= start - first) & (col <= row), 0.0, HIDDEN)
    lane = lax.broadcasted_iota(jnp.int32, (BQ, 128), 1)
    state = [jnp.broadcast_to(start, (BQ, 128))]

    def emit(head, g, mixed, total, top):
        h = head * GROUPS + g
        acc_ref[:, h * DH : (h + 1) * DH] = mixed * (1.0 / total)
        state[0] = jnp.where(lane == HQ + h, total, jnp.where(lane == h, top, state[0]))

    attend(pairs_of(q_ref), heads_of(k_ref), heads_of(v_ref), bias, emit)
    state_ref[...] = state[0]


def back_kernel(first_ref, len_ref, q_ref, k_ref, v_ref, slot_ref):
    first = first_ref[0]
    here = first.astype(jnp.float32)
    keys = k_ref.shape[0]
    block = pl.program_id(0)

    @pl.when((first // keys) % 2 == 0)
    def _():
        ends = document_ends(len_ref[...])
        edge = here + 2 * keys
        start = jnp.max(jnp.where(ends <= edge, ends, 0.0))
        right = jnp.min(jnp.where(ends > edge, ends, edge + edge)) - edge
        by_keys = here + keys - start <= SLOT

        @pl.when(by_keys)
        def _():
            rows = pl.ds(keys - SLOT + block * BQ, BQ)
            slot_ref[:, :KV] = k_ref[rows, :]
            slot_ref[:, KV : 2 * KV] = v_ref[rows, :]
            slot_ref[:, 2 * KV :] = jnp.zeros((BQ, 128), jnp.bfloat16)

        @pl.when(jnp.logical_not(by_keys))
        def _():
            row = float_iota((BQ, 1), 0) + (block * BQ).astype(jnp.float32)
            col = float_iota((BQ, keys), 1)
            bias = jnp.where((col >= start - here) & (row < right), 0.0, HIDDEN)
            lane = lax.broadcasted_iota(jnp.int32, (BQ, 128), 1)
            level = [jnp.zeros((BQ, 128), jnp.float32)]

            def emit(head, g, mixed, total, top):
                h = head * GROUPS + g
                slot_ref[:, h * DH : (h + 1) * DH] = (mixed * (1.0 / total)).astype(jnp.bfloat16)
                level[0] = jnp.where(lane == h, top * RATE + jnp.log2(total), level[0])

            attend(pairs_of(q_ref), heads_of(k_ref), heads_of(v_ref), bias, emit)
            slot_ref[:, 2 * KV :] = in_parts(level[0])


def column(state, lane):
    return state[:, lane : lane + 1]


def heads_lanes(state, group):
    return pltpu.roll(state, 128 - group * HQ, 1) if group else state


def collect(fresh_ref):
    rows = fresh_ref.shape[0]
    lane = lax.broadcasted_iota(jnp.int32, (rows, 128), 1)
    held = [jnp.zeros((rows, 128), jnp.float32)]

    def emit(head, g, mixed, total, top):
        h = head * GROUPS + g
        fresh_ref[:, h * DH : (h + 1) * DH] = mixed
        held[0] = jnp.where(lane == HQ + h, total, jnp.where(lane == h, top, held[0]))

    return emit, held


def joined(state, fresh):
    top = jnp.maximum(state, fresh)
    before = jnp.exp2((state - top) * RATE) * heads_lanes(state, 1)
    take = jnp.exp2((fresh - top) * RATE)
    total = before + take * heads_lanes(fresh, 1)
    scale = 1.0 / total
    return before * scale, take * scale, top, total


def next_kernel(
    first_ref, q_ref, k_ref, v_ref, acc_ref, state_ref, out_ref, new_acc_ref, new_state_ref, fresh_ref, spread_ref
):
    keys = k_ref.shape[0]
    first = first_ref[0].astype(jnp.float32)
    base = first - keys
    state = state_ref[...]
    start = column(state, START)
    lowest = jnp.min(start)

    @pl.when(lowest >= first)
    def _():
        out_ref[...] = acc_ref[...].astype(out_ref.dtype)
        new_state_ref[...] = state

    @pl.when((lowest < first) & (pl.program_id(0) == 0))
    def _():
        spread_ref[...] = spreader()

    @pl.when(lowest < first)
    def _():
        bias = jnp.where(float_iota((BQ, keys), 1) >= start - base, 0.0, HIDDEN)
        emit, held = collect(fresh_ref)
        attend(pairs_of(q_ref), heads_of(k_ref), heads_of(v_ref), bias, emit)
        keep, take, top, total = joined(state, held[0])
        lane = lax.broadcasted_iota(jnp.int32, (BQ, 128), 1)
        totals = pltpu.roll(total, HQ, 1)
        new_state_ref[...] = jnp.where(lane < HQ, top, jnp.where(lane < 2 * HQ, totals, state))

        def write(cols, mixed):
            new_acc_ref[:, cols] = mixed
            out_ref[:, cols] = mixed.astype(out_ref.dtype)

        mix(keep, lambda cols: acc_ref[:, cols], take, lambda cols: fresh_ref[:, cols], spread_ref, write)


def last_kernel(
    first_ref, q_ref, slot_ref, k_ref, v_ref, acc_ref, state_ref, prior_ref, out_ref, rows_ref, fresh_ref,
    spread_ref, sem,
):
    keys = k_ref.shape[0]
    first = first_ref[0].astype(jnp.float32)
    odd = (first_ref[0] // keys) % 2 == 1
    even = jnp.logical_not(odd)
    base = first - keys
    blocks = q_ref.shape[0] // BQ
    by_keys = base - jnp.min(state_ref[:8, START : START + 1]) <= SLOT

    def earliest(block):
        return jnp.min(state_ref[pl.ds(block * BQ, 8), START : START + 1])

    def copy(block):
        rows = pl.ds(pl.multiple_of(block * BQ, BQ), BQ)
        return pltpu.make_async_copy(rows_ref.at[rows, :], out_ref.at[rows, :], sem.at[block])

    def write(rows, keep, take, added):
        def put(cols, mixed):
            rows_ref[rows, cols] = mixed.astype(rows_ref.dtype)

        mix(keep, lambda cols: acc_ref[rows, cols], take, added, spread_ref, put)

    def merge(block, get_keys, get_values, count, origin):
        rows = pl.ds(pl.multiple_of(block * BQ, BQ), BQ)
        state = state_ref[rows, :]
        bias = jnp.where(float_iota((BQ, count), 1) >= column(state, START) - origin, 0.0, HIDDEN)
        emit, held = collect(fresh_ref)
        attend(pairs_of(q_ref, rows), get_keys, get_values, bias, emit)
        keep, take, _, _ = joined(state, held[0])
        write(rows, keep, take, lambda cols: fresh_ref[:, cols])

    def combine(block):
        rows = pl.ds(pl.multiple_of(block * BQ, BQ), BQ)
        state = state_ref[rows, :]
        parts = slot_ref[rows, 2 * KV :].astype(jnp.float32)
        there = sum(heads_lanes(parts, part) for part in reversed(range(PARTS)))
        here = state * RATE
        top = jnp.maximum(here, there)
        before = jnp.exp2(here - top) * heads_lanes(state, 1)
        take = jnp.exp2(there - top)
        scale = 1.0 / (before + take)
        write(rows, before * scale, take * scale, lambda cols: slot_ref[rows, cols])

    @pl.when(earliest(0) < base)
    def _():
        spread_ref[...] = spreader()

    @pl.loop(0, blocks)
    def _(block):
        start = earliest(block)
        needed = start < base
        far = start < base - SLOT

        @pl.when(odd & far)
        def _():
            merge(block, heads_of(k_ref), heads_of(v_ref), keys, base - keys)

        @pl.when(odd & needed & jnp.logical_not(far))
        def _():
            near = slice(keys - SLOT, keys)
            merge(block, heads_of(k_ref, near), heads_of(v_ref, near), SLOT, base - SLOT)

        @pl.when(even & needed & by_keys)
        def _():
            merge(block, heads_of(slot_ref), heads_of(slot_ref, at=KV), SLOT, base - SLOT)

        @pl.when(even & needed & jnp.logical_not(by_keys) & (block * BQ < SLOT))
        def _():
            combine(block)

        @pl.when(needed)
        def _():
            copy(block).start()

    @pl.loop(0, blocks)
    def _(block):
        @pl.when(earliest(block) < base)
        def _():
            copy(block).wait()


def rows_of(width):
    return pl.BlockSpec((BQ, width), lambda i: (i, 0))


SMEM = pl.BlockSpec(memory_space=pltpu.SMEM)
WHOLE = pl.BlockSpec(memory_space=pltpu.VMEM)
WIDE = HQ * DH


def cost(rows, keys):
    return pl.CostEstimate(
        flops=4 * rows * keys * WIDE, bytes_accessed=rows * WIDE * 8, transcendentals=rows * keys * HQ
    )


PARAMS = pltpu.CompilerParams(vmem_limit_bytes=VMEM)


def f32(*shape):
    return jax.ShapeDtypeStruct(shape, jnp.float32)


def bf16(*shape):
    return jax.ShapeDtypeStruct(shape, jnp.bfloat16)


def own_stage(first, lengths, queries, keys, values):
    rows = queries.shape[0]
    return pl.pallas_call(
        own_kernel,
        grid=(rows // BQ,),
        in_specs=[SMEM, WHOLE, rows_of(WIDE), WHOLE, WHOLE],
        out_specs=[rows_of(WIDE), rows_of(128)],
        out_shape=[f32(rows, WIDE), f32(rows, 128)],
        scratch_shapes=[pltpu.VMEM(lengths.shape, jnp.float32)],
        cost_estimate=cost(rows, keys.shape[0]),
        compiler_params=PARAMS,
        name="own_shard",
        interpret=INTERPRET,
    )(first, lengths, queries, keys, values)


def copy_kernel(in_ref, out_ref):
    out_ref[...] = in_ref[...]


def leading_rows(array, rows):
    block = pl.BlockSpec((rows, array.shape[1]), lambda i: (0, 0))
    return pl.pallas_call(
        copy_kernel,
        grid=(1,),
        in_specs=[block],
        out_specs=block,
        out_shape=jax.ShapeDtypeStruct((rows, array.shape[1]), array.dtype),
        compiler_params=PARAMS,
        name="leading_rows",
        interpret=INTERPRET,
    )(array)


def back_stage(first, lengths, queries, keys, values):
    return pl.pallas_call(
        back_kernel,
        grid=(SLOT // BQ,),
        in_specs=[SMEM, WHOLE, rows_of(WIDE), WHOLE, WHOLE],
        out_specs=rows_of(2 * KV + 128),
        out_shape=bf16(SLOT, 2 * KV + 128),
        cost_estimate=cost(SLOT, keys.shape[0]),
        compiler_params=PARAMS,
        name="back_shard",
        interpret=INTERPRET,
    )(first, lengths, queries, keys, values)


def next_stage(first, queries, keys, values, acc, state):
    rows = queries.shape[0]
    return pl.pallas_call(
        next_kernel,
        grid=(rows // BQ,),
        in_specs=[SMEM, rows_of(WIDE), WHOLE, WHOLE, rows_of(WIDE), rows_of(128)],
        out_specs=[rows_of(WIDE), rows_of(WIDE), rows_of(128)],
        out_shape=[bf16(rows, WIDE), f32(rows, WIDE), f32(rows, 128)],
        scratch_shapes=[pltpu.VMEM((BQ, WIDE), jnp.float32), pltpu.VMEM((128, WIDE), jnp.bfloat16)],
        cost_estimate=cost(rows, keys.shape[0]),
        compiler_params=PARAMS,
        name="next_shard",
        interpret=INTERPRET,
    )(first, queries, keys, values, acc, state)


def last_stage(first, queries, slot, keys, values, acc, state, prior):
    rows = queries.shape[0]
    return pl.pallas_call(
        last_kernel,
        in_specs=[SMEM, WHOLE, WHOLE, WHOLE, WHOLE, WHOLE, WHOLE, pl.BlockSpec(memory_space=pl.ANY)],
        out_specs=pl.BlockSpec(memory_space=pl.ANY),
        out_shape=bf16(rows, WIDE),
        scratch_shapes=[
            pltpu.VMEM((rows, WIDE), jnp.bfloat16),
            pltpu.VMEM((BQ, WIDE), jnp.float32),
            pltpu.VMEM((128, WIDE), jnp.bfloat16),
            pltpu.SemaphoreType.DMA((rows // BQ,)),
        ],
        input_output_aliases={7: 0},
        cost_estimate=cost(rows, SLOT),
        compiler_params=PARAMS,
        name="last_shard",
        interpret=INTERPRET,
    )(first, queries, slot, keys, values, acc, state, prior)


def on_device(queries, keys, values, doc_lengths):
    count = lax.axis_size("cp")
    first = (lax.axis_index("cp").astype(jnp.int32) * queries.shape[0]).reshape(1)
    lengths = doc_lengths.reshape(1, -1)
    evens = range(0, count, 2)

    def hop(array, pairs):
        return lax.ppermute(array, "cp", pairs)

    onward = [(i, i + 1) for i in range(count - 1)]
    one_k = hop(keys, onward)
    one_v = hop(values, onward)
    guests = hop(leading_rows(queries, SLOT), [(i, i - 2) for i in evens if i])
    acc, state = own_stage(first, lengths, queries, keys, values)
    slot = back_stage(first, lengths, guests, keys, values)
    slot = hop(slot, [(i, i + 2) for i in evens if i + 2 < count])
    across = [(i, i + 1) for i in evens]
    two_k = hop(one_k, across)
    two_v = hop(one_v, across)
    out, acc, state_next = next_stage(first, queries, one_k, one_v, acc, state)
    out = last_stage(first, queries, slot, two_k, two_v, acc, state_next, out)
    return out


def solution(mesh):
    return jax.shard_map(
        on_device,
        mesh=mesh,
        in_specs=(P(("grp", "cp"), None), P(("grp", "cp"), None), P(("grp", "cp"), None), P("grp")),
        out_specs=P(("grp", "cp"), None),
        check_vma=False,
    )
```

```python
import math

import jax
import jax.numpy as jnp
from jax import lax
from jax.experimental import pallas as pl
from jax.experimental.pallas import tpu as pltpu
from jax.sharding import PartitionSpec as P


HQ = 16
HK = 8
DH = 128
GROUPS = HQ // HK
WIDTH = GROUPS * DH
KV = HK * DH
BQ = 128
HIDDEN = -1e30
RATE = math.log2(math.e) * 144.0 ** -0.5
START = 2 * HQ
PARTS = 3
VMEM = 16 << 20
INTERPRET = False

SLOT = 256


def document_ends(lengths):
    docs = lengths.shape[1]
    sub = lax.broadcasted_iota(jnp.int32, (docs, docs), 0)
    lane = lax.broadcasted_iota(jnp.int32, (docs, docs), 1)
    rows = jnp.broadcast_to(lengths.astype(jnp.float32), (docs, docs))
    column = jnp.sum(jnp.where(sub == lane, rows, 0.0), axis=1, keepdims=True)
    return jnp.sum(jnp.where(sub <= lane, column, 0.0), axis=0, keepdims=True)


def float_iota(shape, axis):
    return lax.broadcasted_iota(jnp.int32, shape, axis).astype(jnp.float32)


def attend(pair, keys, values, bias, emit):
    rows = bias.shape[0]

    def score(head):
        return lax.dot_general(pair(head), keys(head), (((1,), (1,)), ((), ())), preferred_element_type=jnp.float32)

    ahead = score(0)
    for head in range(HK):
        scores = ahead
        if head + 1 < HK:
            ahead = score(head + 1)
        scores = scores.reshape(GROUPS, rows, -1) + bias[None]
        top = jnp.max(scores, axis=-1, keepdims=True)
        weights = jnp.exp2((scores - top) * RATE)
        rounded = weights.astype(jnp.bfloat16).reshape(GROUPS * rows, -1)
        value = values(head)
        value = jnp.concatenate([value, jnp.ones_like(value)], axis=1)
        mixed = lax.dot_general(rounded, value, (((1,), (0,)), ((), ())), preferred_element_type=jnp.float32)
        mixed = mixed.reshape(GROUPS, rows, 2 * DH)
        for g in range(GROUPS):
            emit(head, g, mixed[g, :, :DH], mixed[g, :, DH:], top[g])


def heads_of(ref, rows=slice(None), at=0):
    return lambda head: ref[rows, at + head * DH : at + (head + 1) * DH]


def pairs_of(ref, rows=slice(None)):
    def pair(head):
        both = ref[rows, head * WIDTH : (head + 1) * WIDTH]
        return jnp.concatenate([both[:, :DH], both[:, DH:]], axis=0)

    return pair


def in_parts(table):
    rest = jnp.where(lax.broadcasted_iota(jnp.int32, table.shape, 1) < HQ, table, 0.0)
    parts = jnp.zeros_like(table)
    for part in range(PARTS):
        piece = rest.astype(jnp.bfloat16).astype(jnp.float32)
        parts = parts + (pltpu.roll(piece, part * HQ, 1) if part else piece)
        rest = rest - piece
    return parts.astype(jnp.bfloat16)


def spreader():
    sub = lax.broadcasted_iota(jnp.int32, (128, HQ * DH), 0)
    lane = lax.broadcasted_iota(jnp.int32, (128, HQ * DH), 1)
    return jnp.where((sub < PARTS * HQ) & (sub % HQ == lane // DH), 1.0, 0.0).astype(jnp.bfloat16)


def mix(keep, kept, take, taken, spread_ref, write):
    rows = keep.shape[0]
    table = jnp.concatenate([in_parts(keep), in_parts(take)], axis=0)
    for head in range(HK):
        cols = slice(head * WIDTH, (head + 1) * WIDTH)
        factors = jnp.dot(table, spread_ref[:, cols], preferred_element_type=jnp.float32)
        write(cols, factors[:rows] * kept(cols) + factors[rows:] * taken(cols).astype(jnp.float32))


def own_kernel(first_ref, len_ref, q_ref, k_ref, v_ref, acc_ref, state_ref, spread_ref, out_ref, ends_ref):
    block = pl.program_id(0)

    @pl.when(block == 0)
    def _():
        ends_ref[...] = document_ends(len_ref[...])
        spread_ref[...] = spreader()

    ends = ends_ref[...]
    keys = k_ref.shape[0]
    first = first_ref[0].astype(jnp.float32)
    row = float_iota((BQ, 1), 0) + (block * BQ).astype(jnp.float32)
    start = jnp.max(jnp.where(ends <= row + first, ends, 0.0), axis=1, keepdims=True)
    col = float_iota((BQ, keys), 1)
    bias = jnp.where((col >= start - first) & (col <= row), 0.0, HIDDEN)
    lane = lax.broadcasted_iota(jnp.int32, (BQ, 128), 1)
    state = [jnp.broadcast_to(start, (BQ, 128))]

    def emit(head, g, mixed, total, top):
        h = head * GROUPS + g
        cols = slice(h * DH, (h + 1) * DH)
        mixed = mixed * (1.0 / total)
        acc_ref[:, cols] = mixed
        out_ref[:, cols] = mixed.astype(out_ref.dtype)
        state[0] = jnp.where(lane == HQ + h, total, jnp.where(lane == h, top, state[0]))

    attend(pairs_of(q_ref), heads_of(k_ref), heads_of(v_ref), bias, emit)
    state_ref[...] = state[0]


def back_kernel(first_ref, len_ref, q_ref, k_ref, v_ref, slot_ref):
    first = first_ref[0]
    here = first.astype(jnp.float32)
    keys = k_ref.shape[0]
    block = pl.program_id(0)

    @pl.when((first // keys) % 2 == 0)
    def _():
        ends = document_ends(len_ref[...])
        edge = here + 2 * keys
        start = jnp.max(jnp.where(ends <= edge, ends, 0.0))
        right = jnp.min(jnp.where(ends > edge, ends, edge + edge)) - edge
        reached = start < here + keys
        by_keys = right > SLOT

        @pl.when(reached & by_keys)
        def _():
            rows = pl.ds(keys - SLOT + block * BQ, BQ)
            slot_ref[:, :KV] = k_ref[rows, :]
            slot_ref[:, KV : 2 * KV] = v_ref[rows, :]

        @pl.when(reached & jnp.logical_not(by_keys) & ((block * BQ).astype(jnp.float32) < right))
        def _():
            row = float_iota((BQ, 1), 0) + (block * BQ).astype(jnp.float32)
            col = float_iota((BQ, keys), 1)
            bias = jnp.where((col >= start - here) & (row < right), 0.0, HIDDEN)
            lane = lax.broadcasted_iota(jnp.int32, (BQ, 128), 1)
            level = [jnp.zeros((BQ, 128), jnp.float32)]

            def emit(head, g, mixed, total, top):
                h = head * GROUPS + g
                slot_ref[:, h * DH : (h + 1) * DH] = (mixed * (1.0 / total)).astype(jnp.bfloat16)
                level[0] = jnp.where(lane == h, top * RATE + jnp.log2(total), level[0])

            attend(pairs_of(q_ref), heads_of(k_ref), heads_of(v_ref), bias, emit)
            slot_ref[:, 2 * KV :] = in_parts(level[0])


def column(state, lane):
    return state[:, lane : lane + 1]


def heads_lanes(state, group):
    return pltpu.roll(state, 128 - group * HQ, 1) if group else state


def collect(fresh_ref):
    rows = fresh_ref.shape[0]
    lane = lax.broadcasted_iota(jnp.int32, (rows, 128), 1)
    held = [jnp.zeros((rows, 128), jnp.float32)]

    def emit(head, g, mixed, total, top):
        h = head * GROUPS + g
        fresh_ref[:, h * DH : (h + 1) * DH] = mixed
        held[0] = jnp.where(lane == HQ + h, total, jnp.where(lane == h, top, held[0]))

    return emit, held


def joined(state, fresh):
    top = jnp.maximum(state, fresh)
    before = jnp.exp2((state - top) * RATE) * heads_lanes(state, 1)
    take = jnp.exp2((fresh - top) * RATE)
    total = before + take * heads_lanes(fresh, 1)
    scale = 1.0 / total
    return before * scale, take * scale, top, total


def rows_at(block):
    return pl.ds(pl.multiple_of(block * BQ, BQ), BQ)


def writer(done_ref, out_ref, sem):
    def copy(block):
        return pltpu.make_async_copy(done_ref.at[rows_at(block), :], out_ref.at[rows_at(block), :], sem.at[block])

    return copy


def next_kernel(
    first_ref, q_ref, k_ref, v_ref, acc_ref, state_ref, spread_ref, prior_ref, out_ref, new_acc_ref, new_state_ref,
    done_ref, fresh_ref, sem,
):
    keys = k_ref.shape[0]
    first = first_ref[0].astype(jnp.float32)
    base = first - keys
    blocks = q_ref.shape[0] // BQ
    copy = writer(done_ref, out_ref, sem)

    def earliest(block):
        return jnp.min(state_ref[pl.ds(block * BQ, 8), START : START + 1])

    def finishes(block):
        return (earliest(block) < first) & (earliest(block) >= base)

    @pl.loop(0, blocks)
    def _(block):
        @pl.when(earliest(block) < first)
        def _():
            rows = rows_at(block)
            state = state_ref[rows, :]
            bias = jnp.where(float_iota((BQ, keys), 1) >= column(state, START) - base, 0.0, HIDDEN)
            emit, held = collect(fresh_ref)
            attend(pairs_of(q_ref, rows), heads_of(k_ref), heads_of(v_ref), bias, emit)
            keep, take, top, total = joined(state, held[0])
            lane = lax.broadcasted_iota(jnp.int32, (BQ, 128), 1)
            totals = pltpu.roll(total, HQ, 1)
            new_state_ref[rows, :] = jnp.where(lane < HQ, top, jnp.where(lane < 2 * HQ, totals, state))

            def write(cols, mixed):
                new_acc_ref[rows, cols] = mixed
                done_ref[rows, cols] = mixed.astype(done_ref.dtype)

            mix(keep, lambda cols: acc_ref[rows, cols], take, lambda cols: fresh_ref[:, cols], spread_ref, write)

        @pl.when(finishes(block))
        def _():
            copy(block).start()

    @pl.loop(0, blocks)
    def _(block):
        @pl.when(finishes(block))
        def _():
            copy(block).wait()


def last_kernel(
    first_ref, q_ref, slot_ref, k_ref, v_ref, acc_ref, state_ref, starts_ref, spread_ref, prior_ref, out_ref,
    done_ref, fresh_ref, sem,
):
    keys = k_ref.shape[0]
    first = first_ref[0].astype(jnp.float32)
    odd = (first_ref[0] // keys) % 2 == 1
    even = jnp.logical_not(odd)
    base = first - keys
    blocks = q_ref.shape[0] // BQ
    by_keys = jnp.min(starts_ref[SLOT : SLOT + 8, START : START + 1]) < first
    copy = writer(done_ref, out_ref, sem)

    def earliest(block):
        return jnp.min(starts_ref[pl.ds(block * BQ, 8), START : START + 1])

    def write(rows, keep, take, added):
        def put(cols, mixed):
            done_ref[rows, cols] = mixed.astype(done_ref.dtype)

        mix(keep, lambda cols: acc_ref[rows, cols], take, added, spread_ref, put)

    def merge(block, ref_k, ref_v, at, skip, count, origin):
        rows = rows_at(block)
        state = state_ref[rows, :]
        part = slice(skip, skip + count)
        bias = jnp.where(float_iota((BQ, count), 1) >= column(state, START) - origin, 0.0, HIDDEN)
        emit, held = collect(fresh_ref)
        attend(pairs_of(q_ref, rows), heads_of(ref_k, part), heads_of(ref_v, part, at), bias, emit)
        keep, take, _, _ = joined(state, held[0])
        write(rows, keep, take, lambda cols: fresh_ref[:, cols])

    def combine(block):
        rows = rows_at(block)
        state = state_ref[rows, :]
        parts = slot_ref[rows, 2 * KV :].astype(jnp.float32)
        there = sum(heads_lanes(parts, part) for part in reversed(range(PARTS)))
        here = state * RATE
        top = jnp.maximum(here, there)
        before = jnp.exp2(here - top) * heads_lanes(state, 1)
        take = jnp.exp2(there - top)
        scale = 1.0 / (before + take)
        write(rows, before * scale, take * scale, lambda cols: slot_ref[rows, cols])

    @pl.loop(0, blocks)
    def _(block):
        start = earliest(block)
        needed = start < base
        far = start < base - SLOT
        near = start >= base - BQ

        @pl.when(odd & far)
        def _():
            merge(block, k_ref, v_ref, 0, 0, keys, base - keys)

        @pl.when(odd & needed & jnp.logical_not(far))
        def _():
            merge(block, k_ref, v_ref, 0, keys - SLOT, SLOT, base - SLOT)

        @pl.when(even & needed & by_keys & near)
        def _():
            merge(block, slot_ref, slot_ref, KV, SLOT - BQ, BQ, base - BQ)

        @pl.when(even & needed & by_keys & jnp.logical_not(near))
        def _():
            merge(block, slot_ref, slot_ref, KV, 0, SLOT, base - SLOT)

        @pl.when(even & needed & jnp.logical_not(by_keys) & (block * BQ < SLOT))
        def _():
            combine(block)

        @pl.when(needed)
        def _():
            copy(block).start()

    @pl.loop(0, blocks)
    def _(block):
        @pl.when(earliest(block) < base)
        def _():
            copy(block).wait()


def rows_of(width):
    return pl.BlockSpec((BQ, width), lambda i: (i, 0))


SMEM = pl.BlockSpec(memory_space=pltpu.SMEM)
WHOLE = pl.BlockSpec(memory_space=pltpu.VMEM)
ANY = pl.BlockSpec(memory_space=pl.ANY)
WIDE = HQ * DH


def cost(rows, keys):
    return pl.CostEstimate(
        flops=4 * rows * keys * WIDE, bytes_accessed=rows * WIDE * 8, transcendentals=rows * keys * HQ
    )


PARAMS = pltpu.CompilerParams(vmem_limit_bytes=VMEM)


def f32(*shape):
    return jax.ShapeDtypeStruct(shape, jnp.float32)


def bf16(*shape):
    return jax.ShapeDtypeStruct(shape, jnp.bfloat16)


def own_stage(first, lengths, queries, keys, values):
    rows = queries.shape[0]
    return pl.pallas_call(
        own_kernel,
        grid=(rows // BQ,),
        in_specs=[SMEM, WHOLE, rows_of(WIDE), WHOLE, WHOLE],
        out_specs=[rows_of(WIDE), rows_of(128), WHOLE, rows_of(WIDE)],
        out_shape=[f32(rows, WIDE), f32(rows, 128), bf16(128, WIDE), bf16(rows, WIDE)],
        scratch_shapes=[pltpu.VMEM(lengths.shape, jnp.float32)],
        cost_estimate=cost(rows, keys.shape[0]),
        compiler_params=PARAMS,
        name="own_shard",
        interpret=INTERPRET,
    )(first, lengths, queries, keys, values)


def copy_kernel(in_ref, out_ref):
    out_ref[...] = in_ref[...]


def leading_rows(array, rows):
    block = pl.BlockSpec((rows, array.shape[1]), lambda i: (0, 0))
    return pl.pallas_call(
        copy_kernel,
        grid=(1,),
        in_specs=[block],
        out_specs=block,
        out_shape=jax.ShapeDtypeStruct((rows, array.shape[1]), array.dtype),
        compiler_params=PARAMS,
        name="leading_rows",
        interpret=INTERPRET,
    )(array)


def back_stage(first, lengths, queries, keys, values):
    return pl.pallas_call(
        back_kernel,
        grid=(SLOT // BQ,),
        in_specs=[SMEM, WHOLE, rows_of(WIDE), WHOLE, WHOLE],
        out_specs=rows_of(2 * KV + 128),
        out_shape=bf16(SLOT, 2 * KV + 128),
        cost_estimate=cost(SLOT, keys.shape[0]),
        compiler_params=PARAMS,
        name="back_shard",
        interpret=INTERPRET,
    )(first, lengths, queries, keys, values)


def writing(rows):
    return [
        pltpu.VMEM((rows, WIDE), jnp.bfloat16),
        pltpu.VMEM((BQ, WIDE), jnp.float32),
        pltpu.SemaphoreType.DMA((rows // BQ,)),
    ]


def next_stage(first, queries, keys, values, acc, state, spread, prior):
    rows = queries.shape[0]
    return pl.pallas_call(
        next_kernel,
        in_specs=[SMEM] + [WHOLE] * 6 + [ANY],
        out_specs=[ANY, WHOLE, WHOLE],
        out_shape=[bf16(rows, WIDE), f32(rows, WIDE), f32(rows, 128)],
        scratch_shapes=writing(rows),
        input_output_aliases={7: 0},
        cost_estimate=cost(rows, keys.shape[0]),
        compiler_params=PARAMS,
        name="next_shard",
        interpret=INTERPRET,
    )(first, queries, keys, values, acc, state, spread, prior)


def last_stage(first, queries, slot, keys, values, acc, state, starts, spread, prior):
    rows = queries.shape[0]
    return pl.pallas_call(
        last_kernel,
        in_specs=[SMEM] + [WHOLE] * 8 + [ANY],
        out_specs=ANY,
        out_shape=bf16(rows, WIDE),
        scratch_shapes=writing(rows),
        input_output_aliases={9: 0},
        cost_estimate=cost(rows, SLOT),
        compiler_params=PARAMS,
        name="last_shard",
        interpret=INTERPRET,
    )(first, queries, slot, keys, values, acc, state, starts, spread, prior)


def on_device(queries, keys, values, doc_lengths):
    count = lax.axis_size("cp")
    first = (lax.axis_index("cp").astype(jnp.int32) * queries.shape[0]).reshape(1)
    lengths = doc_lengths.reshape(1, -1)
    evens = range(0, count, 2)

    def hop(array, pairs):
        return lax.ppermute(array, "cp", pairs)

    onward = [(i, i + 1) for i in range(count - 1)]
    one_k = hop(keys, onward)
    one_v = hop(values, onward)
    guests = hop(leading_rows(queries, SLOT), [(i, i - 2) for i in evens if i])
    acc, state, spread, out = own_stage(first, lengths, queries, keys, values)
    slot = back_stage(first, lengths, guests, keys, values)
    slot = hop(slot, [(i, i + 2) for i in evens if i + 2 < count])
    across = [(i, i + 1) for i in evens]
    two_k = hop(one_k, across)
    two_v = hop(one_v, across)
    out, acc, new_state = next_stage(first, queries, one_k, one_v, acc, state, spread, out)
    out = last_stage(first, queries, slot, two_k, two_v, acc, new_state, state, spread, out)
    return out


def solution(mesh):
    return jax.shard_map(
        on_device,
        mesh=mesh,
        in_specs=(P(("grp", "cp"), None), P(("grp", "cp"), None), P(("grp", "cp"), None), P("grp")),
        out_specs=P(("grp", "cp"), None),
        check_vma=False,
    )
```

```python
import functools
import math

import jax
import jax.numpy as jnp
from jax import lax
from jax.experimental import pallas as pl
from jax.experimental.pallas import tpu as pltpu
from jax.sharding import PartitionSpec as P


HQ = 16
HK = 8
DH = 128
GROUPS = HQ // HK
WIDTH = GROUPS * DH
KV = HK * DH
BQ = 128
HIDDEN = -1e30
RATE = math.log2(math.e) * 144.0 ** -0.5
START = 2 * HQ
PARTS = 3
VMEM = 16 << 20
INTERPRET = False

SLOT = 256


def document_ends(lengths):
    docs = lengths.shape[1]
    sub = lax.broadcasted_iota(jnp.int32, (docs, docs), 0)
    lane = lax.broadcasted_iota(jnp.int32, (docs, docs), 1)
    rows = jnp.broadcast_to(lengths.astype(jnp.float32), (docs, docs))
    column = jnp.sum(jnp.where(sub == lane, rows, 0.0), axis=1, keepdims=True)
    return jnp.sum(jnp.where(sub <= lane, column, 0.0), axis=0, keepdims=True)


def float_iota(shape, axis):
    return lax.broadcasted_iota(jnp.int32, shape, axis).astype(jnp.float32)


def attend(pair, keys, values, bias, emit):
    rows = bias.shape[0]

    def score(head):
        return lax.dot_general(pair(head), keys(head), (((1,), (1,)), ((), ())), preferred_element_type=jnp.float32)

    ahead = score(0)
    for head in range(HK):
        scores = ahead
        if head + 1 < HK:
            ahead = score(head + 1)
        scores = scores.reshape(GROUPS, rows, -1) + bias[None]
        top = jnp.max(scores, axis=-1, keepdims=True)
        weights = jnp.exp2((scores - top) * RATE)
        rounded = weights.astype(jnp.bfloat16).reshape(GROUPS * rows, -1)
        value = values(head)
        value = jnp.concatenate([value, jnp.ones_like(value)], axis=1)
        mixed = lax.dot_general(rounded, value, (((1,), (0,)), ((), ())), preferred_element_type=jnp.float32)
        mixed = mixed.reshape(GROUPS, rows, 2 * DH)
        for g in range(GROUPS):
            emit(head, g, mixed[g, :, :DH], mixed[g, :, DH:], top[g])


def heads_of(ref, rows=slice(None), at=0):
    return lambda head: ref[rows, at + head * DH : at + (head + 1) * DH]


def pairs_of(ref, rows=slice(None)):
    def pair(head):
        both = ref[rows, head * WIDTH : (head + 1) * WIDTH]
        return jnp.concatenate([both[:, :DH], both[:, DH:]], axis=0)

    return pair


def in_parts(table):
    rest = jnp.where(lax.broadcasted_iota(jnp.int32, table.shape, 1) < HQ, table, 0.0)
    parts = jnp.zeros_like(table)
    for part in range(PARTS):
        piece = rest.astype(jnp.bfloat16).astype(jnp.float32)
        parts = parts + (pltpu.roll(piece, part * HQ, 1) if part else piece)
        rest = rest - piece
    return parts.astype(jnp.bfloat16)


def spreader():
    sub = lax.broadcasted_iota(jnp.int32, (128, HQ * DH), 0)
    lane = lax.broadcasted_iota(jnp.int32, (128, HQ * DH), 1)
    return jnp.where((sub < PARTS * HQ) & (sub % HQ == lane // DH), 1.0, 0.0).astype(jnp.bfloat16)


def mix(keep, kept, take, taken, spread_ref, write):
    rows = keep.shape[0]
    table = jnp.concatenate([in_parts(keep), in_parts(take)], axis=0)
    for head in range(HK):
        cols = slice(head * WIDTH, (head + 1) * WIDTH)
        factors = jnp.dot(table, spread_ref[:, cols], preferred_element_type=jnp.float32)
        write(cols, factors[:rows] * kept(cols) + factors[rows:] * taken(cols).astype(jnp.float32))


def own_kernel(
    first_ref, len_ref, q_ref, k_ref, v_ref, acc_ref, state_ref, spread_ref, out_ref, mark_ref, ends_ref
):
    block = pl.program_id(0)

    @pl.when(block == 0)
    def _():
        ends_ref[...] = document_ends(len_ref[...])
        spread_ref[...] = spreader()

    ends = ends_ref[...]
    first = first_ref[0].astype(jnp.float32)
    row = float_iota((BQ, 1), 0) + (block * BQ).astype(jnp.float32)
    start = jnp.max(jnp.where(ends <= row + first, ends, 0.0), axis=1, keepdims=True)
    mark_ref[block] = jnp.min(start)
    lane = lax.broadcasted_iota(jnp.int32, (BQ, 128), 1)

    def over(count):
        col = float_iota((BQ, count), 1)
        bias = jnp.where((col >= start - first) & (col <= row), 0.0, HIDDEN)
        state = [jnp.broadcast_to(start, (BQ, 128))]

        def emit(head, g, mixed, total, top):
            h = head * GROUPS + g
            cols = slice(h * DH, (h + 1) * DH)
            mixed = mixed * (1.0 / total)
            acc_ref[:, cols] = mixed
            out_ref[:, cols] = mixed.astype(out_ref.dtype)
            state[0] = jnp.where(lane == HQ + h, total, jnp.where(lane == h, top, state[0]))

        part = slice(0, count)
        attend(pairs_of(q_ref), heads_of(k_ref, part), heads_of(v_ref, part), bias, emit)
        state_ref[...] = state[0]

    for step in range(k_ref.shape[0] // BQ):
        pl.when(block == step)(functools.partial(over, (step + 1) * BQ))


def back_kernel(first_ref, len_ref, q_ref, k_ref, v_ref, slot_ref):
    first = first_ref[0]
    here = first.astype(jnp.float32)
    keys = k_ref.shape[0]
    block = pl.program_id(0)

    @pl.when((first // keys) % 2 == 0)
    def _():
        ends = document_ends(len_ref[...])
        edge = here + 2 * keys
        start = jnp.max(jnp.where(ends <= edge, ends, 0.0))
        right = jnp.min(jnp.where(ends > edge, ends, edge + edge)) - edge
        reached = start < here + keys
        by_keys = right > SLOT

        @pl.when(reached & by_keys)
        def _():
            rows = pl.ds(keys - SLOT + block * BQ, BQ)
            slot_ref[:, :KV] = k_ref[rows, :]
            slot_ref[:, KV : 2 * KV] = v_ref[rows, :]

        def over(count):
            row = float_iota((BQ, 1), 0) + (block * BQ).astype(jnp.float32)
            col = float_iota((BQ, count), 1)
            bias = jnp.where((col >= start - (here + keys - count)) & (row < right), 0.0, HIDDEN)
            lane = lax.broadcasted_iota(jnp.int32, (BQ, 128), 1)
            level = [jnp.zeros((BQ, 128), jnp.float32)]

            def emit(head, g, mixed, total, top):
                h = head * GROUPS + g
                slot_ref[:, h * DH : (h + 1) * DH] = (mixed * (1.0 / total)).astype(jnp.bfloat16)
                level[0] = jnp.where(lane == h, top * RATE + jnp.log2(total), level[0])

            part = slice(keys - count, keys)
            attend(pairs_of(q_ref), heads_of(k_ref, part), heads_of(v_ref, part), bias, emit)
            slot_ref[:, 2 * KV :] = in_parts(level[0])

        working = reached & jnp.logical_not(by_keys) & ((block * BQ).astype(jnp.float32) < right)
        length = here + keys - start
        pl.when(working & (length <= 256))(functools.partial(over, 256))
        pl.when(working & (length > 256) & (length <= 384))(functools.partial(over, 384))
        pl.when(working & (length > 384))(functools.partial(over, keys))


def column(state, lane):
    return state[:, lane : lane + 1]


def heads_lanes(state, group):
    return pltpu.roll(state, 128 - group * HQ, 1) if group else state


def collect(fresh_ref, rows=BQ):
    lane = lax.broadcasted_iota(jnp.int32, (rows, 128), 1)
    held = [jnp.zeros((rows, 128), jnp.float32)]

    def emit(head, g, mixed, total, top):
        h = head * GROUPS + g
        fresh_ref[:rows, h * DH : (h + 1) * DH] = mixed
        held[0] = jnp.where(lane == HQ + h, total, jnp.where(lane == h, top, held[0]))

    return emit, held


def joined(state, fresh):
    top = jnp.maximum(state, fresh)
    before = jnp.exp2((state - top) * RATE) * heads_lanes(state, 1)
    take = jnp.exp2((fresh - top) * RATE)
    total = before + take * heads_lanes(fresh, 1)
    scale = 1.0 / total
    return before * scale, take * scale, top, total


def rows_at(block):
    return pl.ds(pl.multiple_of(block * BQ, BQ), BQ)


def writer(done_ref, out_ref, sem):
    def copy(block):
        return pltpu.make_async_copy(done_ref.at[rows_at(block), :], out_ref.at[rows_at(block), :], sem.at[block])

    return copy


def next_kernel(
    first_ref, mark_ref, q_ref, k_ref, v_ref, acc_ref, state_ref, spread_ref, prior_ref, out_ref, new_acc_ref, new_state_ref,
    done_ref, fresh_ref, sem,
):
    keys = k_ref.shape[0]
    first = first_ref[0].astype(jnp.float32)
    base = first - keys
    blocks = q_ref.shape[0] // BQ
    copy = writer(done_ref, out_ref, sem)

    def finishes(block):
        return (mark_ref[block] < first) & (mark_ref[block] >= base)

    @pl.loop(0, blocks)
    def _(block):
        @pl.when(mark_ref[block] < first)
        def _():
            rows = rows_at(block)
            state = state_ref[rows, :]
            bias = jnp.where(float_iota((BQ, keys), 1) >= column(state, START) - base, 0.0, HIDDEN)
            emit, held = collect(fresh_ref)
            attend(pairs_of(q_ref, rows), heads_of(k_ref), heads_of(v_ref), bias, emit)
            keep, take, top, total = joined(state, held[0])
            lane = lax.broadcasted_iota(jnp.int32, (BQ, 128), 1)
            totals = pltpu.roll(total, HQ, 1)
            new_state_ref[rows, :] = jnp.where(lane < HQ, top, jnp.where(lane < 2 * HQ, totals, state))

            def write(cols, mixed):
                new_acc_ref[rows, cols] = mixed
                done_ref[rows, cols] = mixed.astype(done_ref.dtype)

            mix(keep, lambda cols: acc_ref[rows, cols], take, lambda cols: fresh_ref[:BQ, cols], spread_ref, write)

        @pl.when(finishes(block))
        def _():
            copy(block).start()

    @pl.loop(0, blocks)
    def _(block):
        @pl.when(finishes(block))
        def _():
            copy(block).wait()


def last_kernel(
    first_ref, mark_ref, q_ref, slot_ref, k_ref, v_ref, acc_ref, state_ref, spread_ref, prior_ref, out_ref,
    done_ref, fresh_ref, sem,
):
    keys = k_ref.shape[0]
    first = first_ref[0].astype(jnp.float32)
    odd = (first_ref[0] // keys) % 2 == 1
    even = jnp.logical_not(odd)
    base = first - keys
    blocks = q_ref.shape[0] // BQ
    start = mark_ref[0]
    by_keys = mark_ref[SLOT // BQ] < first
    copy = writer(done_ref, out_ref, sem)

    def write(rows, keep, take, added):
        def put(cols, mixed):
            done_ref[rows, cols] = mixed.astype(done_ref.dtype)

        mix(keep, lambda cols: acc_ref[rows, cols], take, added, spread_ref, put)

    def merge(block, tall, ref_k, ref_v, at, count):
        rows = pl.ds(pl.multiple_of(block * BQ, BQ), tall * BQ)
        state = state_ref[rows, :]
        skip = ref_k.shape[0] - count
        part = slice(skip, skip + count)
        bias = jnp.where(float_iota((tall * BQ, count), 1) >= column(state, START) - (base - count), 0.0, HIDDEN)
        emit, held = collect(fresh_ref, tall * BQ)
        attend(pairs_of(q_ref, rows), heads_of(ref_k, part), heads_of(ref_v, part, at), bias, emit)
        keep, take, _, _ = joined(state, held[0])
        write(rows, keep, take, lambda cols: fresh_ref[: tall * BQ, cols])

    def combine(block):
        rows = rows_at(block)
        state = state_ref[rows, :]
        parts = slot_ref[rows, 2 * KV :].astype(jnp.float32)
        there = sum(heads_lanes(parts, part) for part in reversed(range(PARTS)))
        here = state * RATE
        top = jnp.maximum(here, there)
        before = jnp.exp2(here - top) * heads_lanes(state, 1)
        take = jnp.exp2(there - top)
        scale = 1.0 / (before + take)
        write(rows, before * scale, take * scale, lambda cols: slot_ref[rows, cols])

    def sweep(condition, tall, work, end=blocks):
        @pl.when(condition & (start < base))
        def _():
            @pl.loop(0, end // tall)
            def _(step):
                block = step * tall

                @pl.when(mark_ref[block] < base)
                def _():
                    work(block)
                    for i in range(tall):
                        pl.when(mark_ref[block + i] < base)(copy(block + i).start)

    near = start >= base - BQ
    far = start < base - SLOT
    some = jnp.logical_not(near | far)
    sweep(odd & near, 2, lambda block: merge(block, 2, k_ref, v_ref, 0, BQ))
    sweep(odd & some, 1, lambda block: merge(block, 1, k_ref, v_ref, 0, SLOT))
    sweep(odd & far, 1, lambda block: merge(block, 1, k_ref, v_ref, 0, keys))
    sweep(even & by_keys & near, 2, lambda block: merge(block, 2, slot_ref, slot_ref, KV, BQ))
    sweep(even & by_keys & jnp.logical_not(near), 1, lambda block: merge(block, 1, slot_ref, slot_ref, KV, SLOT))
    sweep(even & jnp.logical_not(by_keys), 1, combine, SLOT // BQ)

    @pl.loop(0, blocks)
    def _(block):
        pl.when(mark_ref[block] < base)(lambda: copy(block).wait())


def rows_of(width):
    return pl.BlockSpec((BQ, width), lambda i: (i, 0))


SMEM = pl.BlockSpec(memory_space=pltpu.SMEM)
WHOLE = pl.BlockSpec(memory_space=pltpu.VMEM)
ANY = pl.BlockSpec(memory_space=pl.ANY)
WIDE = HQ * DH


def cost(rows, keys):
    return pl.CostEstimate(
        flops=4 * rows * keys * WIDE, bytes_accessed=rows * WIDE * 8, transcendentals=rows * keys * HQ
    )


PARAMS = pltpu.CompilerParams(vmem_limit_bytes=VMEM)


def f32(*shape):
    return jax.ShapeDtypeStruct(shape, jnp.float32)


def bf16(*shape):
    return jax.ShapeDtypeStruct(shape, jnp.bfloat16)


def own_stage(first, lengths, queries, keys, values):
    rows = queries.shape[0]
    return pl.pallas_call(
        own_kernel,
        grid=(rows // BQ,),
        in_specs=[SMEM, WHOLE, rows_of(WIDE), WHOLE, WHOLE],
        out_specs=[rows_of(WIDE), rows_of(128), WHOLE, rows_of(WIDE), SMEM],
        out_shape=[f32(rows, WIDE), f32(rows, 128), bf16(128, WIDE), bf16(rows, WIDE), f32(rows // BQ)],
        scratch_shapes=[pltpu.VMEM(lengths.shape, jnp.float32)],
        cost_estimate=cost(rows, keys.shape[0]),
        compiler_params=PARAMS,
        name="own_shard",
        interpret=INTERPRET,
    )(first, lengths, queries, keys, values)


def copy_kernel(in_ref, out_ref, sem):
    copy = pltpu.make_async_copy(in_ref.at[pl.ds(0, out_ref.shape[0]), :], out_ref, sem)
    copy.start()
    copy.wait()


def leading_rows(array, rows):
    return pl.pallas_call(
        copy_kernel,
        in_specs=[pl.BlockSpec(memory_space=pltpu.HBM)],
        out_specs=WHOLE,
        out_shape=jax.ShapeDtypeStruct((rows, array.shape[1]), array.dtype),
        scratch_shapes=[pltpu.SemaphoreType.DMA],
        compiler_params=PARAMS,
        name="leading_rows",
        interpret=INTERPRET,
    )(pltpu.with_memory_space_constraint(array, pltpu.HBM))


def back_stage(first, lengths, queries, keys, values):
    return pl.pallas_call(
        back_kernel,
        grid=(SLOT // BQ,),
        in_specs=[SMEM, WHOLE, rows_of(WIDE), WHOLE, WHOLE],
        out_specs=rows_of(2 * KV + 128),
        out_shape=bf16(SLOT, 2 * KV + 128),
        cost_estimate=cost(SLOT, keys.shape[0]),
        compiler_params=PARAMS,
        name="back_shard",
        interpret=INTERPRET,
    )(first, lengths, queries, keys, values)


def writing(rows):
    return [
        pltpu.VMEM((rows, WIDE), jnp.bfloat16),
        pltpu.VMEM((2 * BQ, WIDE), jnp.float32),
        pltpu.SemaphoreType.DMA((rows // BQ,)),
    ]


def next_stage(first, marks, queries, keys, values, acc, state, spread, prior):
    rows = queries.shape[0]
    return pl.pallas_call(
        next_kernel,
        in_specs=[SMEM] * 2 + [WHOLE] * 6 + [ANY],
        out_specs=[ANY, WHOLE, WHOLE],
        out_shape=[bf16(rows, WIDE), f32(rows, WIDE), f32(rows, 128)],
        scratch_shapes=writing(rows),
        input_output_aliases={8: 0},
        cost_estimate=cost(rows, keys.shape[0]),
        compiler_params=PARAMS,
        name="next_shard",
        interpret=INTERPRET,
    )(first, marks, queries, keys, values, acc, state, spread, prior)


def last_stage(first, marks, queries, slot, keys, values, acc, state, spread, prior):
    rows = queries.shape[0]
    return pl.pallas_call(
        last_kernel,
        in_specs=[SMEM] * 2 + [WHOLE] * 7 + [ANY],
        out_specs=ANY,
        out_shape=bf16(rows, WIDE),
        scratch_shapes=writing(rows),
        input_output_aliases={9: 0},
        cost_estimate=cost(rows, SLOT),
        compiler_params=PARAMS,
        name="last_shard",
        interpret=INTERPRET,
    )(first, marks, queries, slot, keys, values, acc, state, spread, prior)


def on_device(queries, keys, values, doc_lengths):
    count = lax.axis_size("cp")
    first = (lax.axis_index("cp").astype(jnp.int32) * queries.shape[0]).reshape(1)
    lengths = doc_lengths.reshape(1, -1)
    evens = range(0, count, 2)

    def hop(array, pairs):
        return lax.ppermute(array, "cp", pairs)

    onward = [(i, i + 1) for i in range(count - 1)]
    one_k = hop(keys, onward)
    one_v = hop(values, onward)
    guests = hop(leading_rows(queries, SLOT), [(i, i - 2) for i in evens if i])
    acc, state, spread, out, marks = own_stage(first, lengths, queries, keys, values)
    slot = back_stage(first, lengths, guests, keys, values)
    slot = hop(slot, [(i, i + 2) for i in evens if i + 2 < count])
    across = [(i, i + 1) for i in evens]
    two_k = hop(one_k, across)
    two_v = hop(one_v, across)
    out, acc, new_state = next_stage(first, marks, queries, one_k, one_v, acc, state, spread, out)
    out = last_stage(first, marks, queries, slot, two_k, two_v, acc, new_state, spread, out)
    return out


def solution(mesh):
    return jax.shard_map(
        on_device,
        mesh=mesh,
        in_specs=(P(("grp", "cp"), None), P(("grp", "cp"), None), P(("grp", "cp"), None), P("grp")),
        out_specs=P(("grp", "cp"), None),
        check_vma=False,
    )
```

```python
import functools
import math

import jax
import jax.numpy as jnp
from jax import lax
from jax.experimental import pallas as pl
from jax.experimental.pallas import tpu as pltpu
from jax.sharding import PartitionSpec as P


HQ = 16
HK = 8
DH = 128
GROUPS = HQ // HK
WIDTH = GROUPS * DH
KV = HK * DH
BQ = 128
HIDDEN = -1e30
RATE = math.log2(math.e) * 144.0 ** -0.5
START = 2 * HQ
PARTS = 3
VMEM = 16 << 20
FEW = 128
INTERPRET = False

SLOT = 256


def document_ends(lengths):
    docs = lengths.shape[1]
    sub = lax.broadcasted_iota(jnp.int32, (docs, docs), 0)
    lane = lax.broadcasted_iota(jnp.int32, (docs, docs), 1)
    rows = jnp.broadcast_to(lengths.astype(jnp.float32), (docs, docs))
    column = jnp.sum(jnp.where(sub == lane, rows, 0.0), axis=1, keepdims=True)
    return jnp.sum(jnp.where(sub <= lane, column, 0.0), axis=0, keepdims=True)


def float_iota(shape, axis):
    return lax.broadcasted_iota(jnp.int32, shape, axis).astype(jnp.float32)


def attend(pair, keys, values, bias, emit):
    rows = bias.shape[0]

    def score(head):
        return lax.dot_general(pair(head), keys(head), (((1,), (1,)), ((), ())), preferred_element_type=jnp.float32)

    ahead = score(0)
    for head in range(HK):
        scores = ahead
        if head + 1 < HK:
            ahead = score(head + 1)
        scores = scores.reshape(GROUPS, rows, -1) + bias[None]
        top = jnp.max(scores, axis=-1, keepdims=True)
        weights = jnp.exp2((scores - top) * RATE)
        rounded = weights.astype(jnp.bfloat16).reshape(GROUPS * rows, -1)
        value = values(head)
        few = value.shape[0] <= FEW
        if not few:
            value = jnp.concatenate([value, jnp.ones_like(value)], axis=1)
        mixed = lax.dot_general(rounded, value, (((1,), (0,)), ((), ())), preferred_element_type=jnp.float32)
        mixed = mixed.reshape(GROUPS, rows, -1)
        totals = jnp.sum(weights, axis=-1, keepdims=True) if few else mixed[:, :, DH:]
        for g in range(GROUPS):
            emit(head, g, mixed[g, :, :DH], totals[g], top[g])


def heads_of(ref, rows=slice(None), at=0):
    return lambda head: ref[rows, at + head * DH : at + (head + 1) * DH]


def pairs_of(ref, rows=slice(None)):
    def pair(head):
        both = ref[rows, head * WIDTH : (head + 1) * WIDTH]
        return jnp.concatenate([both[:, :DH], both[:, DH:]], axis=0)

    return pair


def in_parts(table):
    rest = jnp.where(lax.broadcasted_iota(jnp.int32, table.shape, 1) < HQ, table, 0.0)
    parts = jnp.zeros_like(table)
    for part in range(PARTS):
        piece = rest.astype(jnp.bfloat16).astype(jnp.float32)
        parts = parts + (pltpu.roll(piece, part * HQ, 1) if part else piece)
        rest = rest - piece
    return parts.astype(jnp.bfloat16)


def spreader():
    sub = lax.broadcasted_iota(jnp.int32, (128, HQ * DH), 0)
    lane = lax.broadcasted_iota(jnp.int32, (128, HQ * DH), 1)
    return jnp.where((sub < PARTS * HQ) & (sub % HQ == lane // DH), 1.0, 0.0).astype(jnp.bfloat16)


def mix(keep, kept, take, taken, spread_ref, write):
    rows = keep.shape[0]
    table = jnp.concatenate([in_parts(keep), in_parts(take)], axis=0)
    for head in range(HK):
        cols = slice(head * WIDTH, (head + 1) * WIDTH)
        factors = jnp.dot(table, spread_ref[:, cols], preferred_element_type=jnp.float32)
        write(cols, factors[:rows] * kept(cols) + factors[rows:] * taken(cols).astype(jnp.float32))


def own_kernel(
    first_ref, len_ref, q_ref, k_ref, v_ref, acc_ref, state_ref, spread_ref, out_ref, mark_ref, ends_ref
):
    block = pl.program_id(0)

    @pl.when(block == 0)
    def _():
        ends_ref[...] = document_ends(len_ref[...])
        spread_ref[...] = spreader()

    ends = ends_ref[...]
    first = first_ref[0].astype(jnp.float32)
    row = float_iota((BQ, 1), 0) + (block * BQ).astype(jnp.float32)
    start = jnp.max(jnp.where(ends <= row + first, ends, 0.0), axis=1, keepdims=True)
    mark_ref[block] = jnp.min(start)
    lane = lax.broadcasted_iota(jnp.int32, (BQ, 128), 1)

    def over(count):
        col = float_iota((BQ, count), 1)
        bias = jnp.where((col >= start - first) & (col <= row), 0.0, HIDDEN)
        state = [jnp.broadcast_to(start, (BQ, 128))]

        def emit(head, g, mixed, total, top):
            h = head * GROUPS + g
            cols = slice(h * DH, (h + 1) * DH)
            mixed = mixed * (1.0 / total)
            acc_ref[:, cols] = mixed
            out_ref[:, cols] = mixed.astype(out_ref.dtype)
            state[0] = jnp.where(lane == HQ + h, total, jnp.where(lane == h, top, state[0]))

        part = slice(0, count)
        attend(pairs_of(q_ref), heads_of(k_ref, part), heads_of(v_ref, part), bias, emit)
        state_ref[...] = state[0]

    for step in range(k_ref.shape[0] // BQ):
        pl.when(block == step)(functools.partial(over, (step + 1) * BQ))


def back_kernel(first_ref, len_ref, q_ref, k_ref, v_ref, slot_ref):
    first = first_ref[0]
    here = first.astype(jnp.float32)
    keys = k_ref.shape[0]
    block = pl.program_id(0)

    @pl.when((first // keys) % 2 == 0)
    def _():
        ends = document_ends(len_ref[...])
        edge = here + 2 * keys
        start = jnp.max(jnp.where(ends <= edge, ends, 0.0))
        right = jnp.min(jnp.where(ends > edge, ends, edge + edge)) - edge
        reached = start < here + keys
        by_keys = right > SLOT

        @pl.when(reached & by_keys)
        def _():
            rows = pl.ds(keys - SLOT + block * BQ, BQ)
            slot_ref[:, :KV] = k_ref[rows, :]
            slot_ref[:, KV : 2 * KV] = v_ref[rows, :]

        def over(count):
            row = float_iota((BQ, 1), 0) + (block * BQ).astype(jnp.float32)
            col = float_iota((BQ, count), 1)
            bias = jnp.where((col >= start - (here + keys - count)) & (row < right), 0.0, HIDDEN)
            lane = lax.broadcasted_iota(jnp.int32, (BQ, 128), 1)
            level = [jnp.zeros((BQ, 128), jnp.float32)]

            def emit(head, g, mixed, total, top):
                h = head * GROUPS + g
                slot_ref[:, h * DH : (h + 1) * DH] = (mixed * (1.0 / total)).astype(jnp.bfloat16)
                level[0] = jnp.where(lane == h, top * RATE + jnp.log2(total), level[0])

            part = slice(keys - count, keys)
            attend(pairs_of(q_ref), heads_of(k_ref, part), heads_of(v_ref, part), bias, emit)
            slot_ref[:, 2 * KV :] = in_parts(level[0])

        working = reached & jnp.logical_not(by_keys) & ((block * BQ).astype(jnp.float32) < right)
        length = here + keys - start
        pl.when(working & (length <= 256))(functools.partial(over, 256))
        pl.when(working & (length > 256) & (length <= 384))(functools.partial(over, 384))
        pl.when(working & (length > 384))(functools.partial(over, keys))


def column(state, lane):
    return state[:, lane : lane + 1]


def heads_lanes(state, group):
    return pltpu.roll(state, 128 - group * HQ, 1) if group else state


def collect(fresh_ref, rows=BQ):
    lane = lax.broadcasted_iota(jnp.int32, (rows, 128), 1)
    held = [jnp.zeros((rows, 128), jnp.float32)]

    def emit(head, g, mixed, total, top):
        h = head * GROUPS + g
        fresh_ref[:rows, h * DH : (h + 1) * DH] = mixed
        held[0] = jnp.where(lane == HQ + h, total, jnp.where(lane == h, top, held[0]))

    return emit, held


def joined(state, fresh):
    top = jnp.maximum(state, fresh)
    before = jnp.exp2((state - top) * RATE) * heads_lanes(state, 1)
    take = jnp.exp2((fresh - top) * RATE)
    total = before + take * heads_lanes(fresh, 1)
    scale = 1.0 / total
    return before * scale, take * scale, top, total


def rows_at(block):
    return pl.ds(pl.multiple_of(block * BQ, BQ), BQ)


def writer(done_ref, out_ref, sem):
    def copy(block):
        return pltpu.make_async_copy(done_ref.at[rows_at(block), :], out_ref.at[rows_at(block), :], sem.at[block])

    return copy


def next_kernel(
    first_ref, mark_ref, q_ref, k_ref, v_ref, acc_ref, state_ref, spread_ref, prior_ref, out_ref, new_acc_ref, new_state_ref,
    done_ref, fresh_all_ref, sem,
):
    keys = k_ref.shape[0]
    first = first_ref[0].astype(jnp.float32)
    base = first - keys
    blocks = q_ref.shape[0] // BQ
    copy = writer(done_ref, out_ref, sem)
    fresh_ref = fresh_all_ref.at[0]

    def finishes(block):
        return (mark_ref[block] < first) & (mark_ref[block] >= base)

    @pl.loop(0, blocks)
    def _(block):
        @pl.when(mark_ref[block] < first)
        def _():
            rows = rows_at(block)
            state = state_ref[rows, :]
            bias = jnp.where(float_iota((BQ, keys), 1) >= column(state, START) - base, 0.0, HIDDEN)
            emit, held = collect(fresh_ref)
            attend(pairs_of(q_ref, rows), heads_of(k_ref), heads_of(v_ref), bias, emit)
            keep, take, top, total = joined(state, held[0])
            lane = lax.broadcasted_iota(jnp.int32, (BQ, 128), 1)
            totals = pltpu.roll(total, HQ, 1)
            new_state_ref[rows, :] = jnp.where(lane < HQ, top, jnp.where(lane < 2 * HQ, totals, state))

            def write(cols, mixed):
                new_acc_ref[rows, cols] = mixed
                done_ref[rows, cols] = mixed.astype(done_ref.dtype)

            mix(keep, lambda cols: acc_ref[rows, cols], take, lambda cols: fresh_ref[:BQ, cols], spread_ref, write)

        @pl.when(finishes(block))
        def _():
            copy(block).start()

    @pl.loop(0, blocks)
    def _(block):
        @pl.when(finishes(block))
        def _():
            copy(block).wait()


def last_kernel(
    first_ref, mark_ref, q_ref, slot_ref, k_ref, v_ref, acc_ref, state_ref, spread_ref, prior_ref, out_ref,
    done_ref, fresh_ref, sem,
):
    keys = k_ref.shape[0]
    first = first_ref[0].astype(jnp.float32)
    odd = (first_ref[0] // keys) % 2 == 1
    even = jnp.logical_not(odd)
    base = first - keys
    blocks = q_ref.shape[0] // BQ
    start = mark_ref[0]
    by_keys = mark_ref[SLOT // BQ] < first
    copy = writer(done_ref, out_ref, sem)

    def write(rows, keep, take, added):
        def put(cols, mixed):
            done_ref[rows, cols] = mixed.astype(done_ref.dtype)

        mix(keep, lambda cols: acc_ref[rows, cols], take, added, spread_ref, put)

    def merge(block, tall, ref_k, ref_v, at, count, fresh):
        rows = pl.ds(pl.multiple_of(block * BQ, BQ), tall * BQ)
        state = state_ref[rows, :]
        skip = ref_k.shape[0] - count
        part = slice(skip, skip + count)
        bias = jnp.where(float_iota((tall * BQ, count), 1) >= column(state, START) - (base - count), 0.0, HIDDEN)
        emit, held = collect(fresh, tall * BQ)
        attend(pairs_of(q_ref, rows), heads_of(ref_k, part), heads_of(ref_v, part, at), bias, emit)

        def finish():
            keep, take, _, _ = joined(state, held[0])
            write(rows, keep, take, lambda cols: fresh[: tall * BQ, cols])
            for i in range(tall):
                pl.when(mark_ref[block + i] < base)(copy(block + i).start)

        return finish

    def combine(block):
        rows = rows_at(block)
        state = state_ref[rows, :]
        parts = slot_ref[rows, 2 * KV :].astype(jnp.float32)
        there = sum(heads_lanes(parts, part) for part in reversed(range(PARTS)))
        here = state * RATE
        top = jnp.maximum(here, there)
        before = jnp.exp2(here - top) * heads_lanes(state, 1)
        take = jnp.exp2(there - top)
        scale = 1.0 / (before + take)
        write(rows, before * scale, take * scale, lambda cols: slot_ref[rows, cols])

    def sweep(condition, tall, work, end=blocks):
        @pl.when(condition & (start < base))
        def _():
            @pl.loop(0, end // tall)
            def _(step):
                block = step * tall

                @pl.when(mark_ref[block] < base)
                def _():
                    work(block)

    near = start >= base - BQ
    far = start < base - SLOT
    some = jnp.logical_not(near | far)
    sweep(odd & near, 2, lambda block: merge(block, 2, k_ref, v_ref, 0, BQ, fresh_ref.at[0])())
    sweep(odd & some, 1, lambda block: merge(block, 1, k_ref, v_ref, 0, SLOT, fresh_ref.at[0])())
    sweep(odd & far, 1, lambda block: merge(block, 1, k_ref, v_ref, 0, keys, fresh_ref.at[0])())

    def with_slot(count):
        pending = None
        for block in range(SLOT // BQ + 1):
            finish = merge(block, 1, slot_ref, slot_ref, KV, count, fresh_ref.at[block % 2])
            if pending is not None:
                pending()
            pending = finish
        pending()
        if count == BQ:
            pl.when(mark_ref[blocks - 1] < base)(
                lambda: merge(blocks - 1, 1, slot_ref, slot_ref, KV, count, fresh_ref.at[1])()
            )

    travelled = even & by_keys & (start < base)
    pl.when(travelled & near)(functools.partial(with_slot, BQ))
    pl.when(travelled & jnp.logical_not(near))(functools.partial(with_slot, SLOT))

    def combined(block):
        combine(block)
        copy(block).start()

    sweep(even & jnp.logical_not(by_keys), 1, combined, SLOT // BQ)

    @pl.loop(0, blocks)
    def _(block):
        pl.when(mark_ref[block] < base)(lambda: copy(block).wait())


def rows_of(width):
    return pl.BlockSpec((BQ, width), lambda i: (i, 0))


SMEM = pl.BlockSpec(memory_space=pltpu.SMEM)
WHOLE = pl.BlockSpec(memory_space=pltpu.VMEM)
ANY = pl.BlockSpec(memory_space=pl.ANY)
WIDE = HQ * DH


def cost(rows, keys):
    return pl.CostEstimate(
        flops=4 * rows * keys * WIDE, bytes_accessed=rows * WIDE * 8, transcendentals=rows * keys * HQ
    )


PARAMS = pltpu.CompilerParams(vmem_limit_bytes=VMEM)


def f32(*shape):
    return jax.ShapeDtypeStruct(shape, jnp.float32)


def bf16(*shape):
    return jax.ShapeDtypeStruct(shape, jnp.bfloat16)


def own_stage(first, lengths, queries, keys, values):
    rows = queries.shape[0]
    return pl.pallas_call(
        own_kernel,
        grid=(rows // BQ,),
        in_specs=[SMEM, WHOLE, rows_of(WIDE), WHOLE, WHOLE],
        out_specs=[rows_of(WIDE), rows_of(128), WHOLE, rows_of(WIDE), SMEM],
        out_shape=[f32(rows, WIDE), f32(rows, 128), bf16(128, WIDE), bf16(rows, WIDE), f32(rows // BQ)],
        scratch_shapes=[pltpu.VMEM(lengths.shape, jnp.float32)],
        cost_estimate=cost(rows, keys.shape[0]),
        compiler_params=PARAMS,
        name="own_shard",
        interpret=INTERPRET,
    )(first, lengths, queries, keys, values)


def copy_kernel(in_ref, out_ref, sem):
    copy = pltpu.make_async_copy(in_ref.at[pl.ds(0, out_ref.shape[0]), :], out_ref, sem)
    copy.start()
    copy.wait()


def leading_rows(array, rows):
    return pl.pallas_call(
        copy_kernel,
        in_specs=[pl.BlockSpec(memory_space=pltpu.HBM)],
        out_specs=WHOLE,
        out_shape=jax.ShapeDtypeStruct((rows, array.shape[1]), array.dtype),
        scratch_shapes=[pltpu.SemaphoreType.DMA],
        compiler_params=PARAMS,
        name="leading_rows",
        interpret=INTERPRET,
    )(pltpu.with_memory_space_constraint(array, pltpu.HBM))


def back_stage(first, lengths, queries, keys, values):
    return pl.pallas_call(
        back_kernel,
        grid=(SLOT // BQ,),
        in_specs=[SMEM, WHOLE, rows_of(WIDE), WHOLE, WHOLE],
        out_specs=rows_of(2 * KV + 128),
        out_shape=bf16(SLOT, 2 * KV + 128),
        cost_estimate=cost(SLOT, keys.shape[0]),
        compiler_params=PARAMS,
        name="back_shard",
        interpret=INTERPRET,
    )(first, lengths, queries, keys, values)


def writing(rows):
    return [
        pltpu.VMEM((rows, WIDE), jnp.bfloat16),
        pltpu.VMEM((2, 2 * BQ, WIDE), jnp.float32),
        pltpu.SemaphoreType.DMA((rows // BQ,)),
    ]


def next_stage(first, marks, queries, keys, values, acc, state, spread, prior):
    rows = queries.shape[0]
    return pl.pallas_call(
        next_kernel,
        in_specs=[SMEM] * 2 + [WHOLE] * 6 + [ANY],
        out_specs=[ANY, WHOLE, WHOLE],
        out_shape=[bf16(rows, WIDE), f32(rows, WIDE), f32(rows, 128)],
        scratch_shapes=writing(rows),
        input_output_aliases={8: 0},
        cost_estimate=cost(rows, keys.shape[0]),
        compiler_params=PARAMS,
        name="next_shard",
        interpret=INTERPRET,
    )(first, marks, queries, keys, values, acc, state, spread, prior)


def last_stage(first, marks, queries, slot, keys, values, acc, state, spread, prior):
    rows = queries.shape[0]
    return pl.pallas_call(
        last_kernel,
        in_specs=[SMEM] * 2 + [WHOLE] * 7 + [ANY],
        out_specs=ANY,
        out_shape=bf16(rows, WIDE),
        scratch_shapes=writing(rows),
        input_output_aliases={9: 0},
        cost_estimate=cost(rows, SLOT),
        compiler_params=PARAMS,
        name="last_shard",
        interpret=INTERPRET,
    )(first, marks, queries, slot, keys, values, acc, state, spread, prior)


def on_device(queries, keys, values, doc_lengths):
    count = lax.axis_size("cp")
    first = (lax.axis_index("cp").astype(jnp.int32) * queries.shape[0]).reshape(1)
    lengths = doc_lengths.reshape(1, -1)
    evens = range(0, count, 2)

    def hop(array, pairs):
        return lax.ppermute(array, "cp", pairs)

    onward = [(i, i + 1) for i in range(count - 1)]
    one_k = hop(keys, onward)
    one_v = hop(values, onward)
    guests = hop(leading_rows(queries, SLOT), [(i, i - 2) for i in evens if i])
    acc, state, spread, out, marks = own_stage(first, lengths, queries, keys, values)
    slot = back_stage(first, lengths, guests, keys, values)
    slot = hop(slot, [(i, i + 2) for i in evens if i + 2 < count])
    across = [(i, i + 1) for i in evens]
    two_k = hop(one_k, across)
    two_v = hop(one_v, across)
    out, acc, new_state = next_stage(first, marks, queries, one_k, one_v, acc, state, spread, out)
    out = last_stage(first, marks, queries, slot, two_k, two_v, acc, new_state, spread, out)
    return out


def solution(mesh):
    return jax.shard_map(
        on_device,
        mesh=mesh,
        in_specs=(P(("grp", "cp"), None), P(("grp", "cp"), None), P(("grp", "cp"), None), P("grp")),
        out_specs=P(("grp", "cp"), None),
        check_vma=False,
    )
```

```python
import functools
import math

import jax
import jax.numpy as jnp
from jax import lax
from jax.experimental import pallas as pl
from jax.experimental.pallas import tpu as pltpu
from jax.sharding import PartitionSpec as P


HQ = 16
HK = 8
DH = 128
GROUPS = HQ // HK
WIDTH = GROUPS * DH
KV = HK * DH
BQ = 128
HIDDEN = -1e30
RATE = math.log2(math.e) * 144.0 ** -0.5
PARTS = 3
VMEM = 16 << 20
FEW = 128
INTERPRET = False

SLOT = 256


def document_ends(lengths):
    docs = lengths.shape[1]
    sub = lax.broadcasted_iota(jnp.int32, (docs, docs), 0)
    lane = lax.broadcasted_iota(jnp.int32, (docs, docs), 1)
    rows = jnp.broadcast_to(lengths.astype(jnp.float32), (docs, docs))
    column = jnp.sum(jnp.where(sub == lane, rows, 0.0), axis=1, keepdims=True)
    return jnp.sum(jnp.where(sub <= lane, column, 0.0), axis=0, keepdims=True)


def float_iota(shape, axis):
    return lax.broadcasted_iota(jnp.int32, shape, axis).astype(jnp.float32)


def attend(pair, keys, values, bias, emit, before=None):
    rows = bias.shape[0]

    def score(head):
        return lax.dot_general(pair(head), keys(head), (((1,), (1,)), ((), ())), preferred_element_type=jnp.float32)

    ahead = score(0)
    for head in range(HK):
        scores = ahead
        if head + 1 < HK:
            ahead = score(head + 1)
        scores = scores.reshape(GROUPS, rows, -1) + bias[None]
        top = jnp.max(scores, axis=-1, keepdims=True)
        if before is not None:
            top = jnp.maximum(top, jnp.stack([before(head * GROUPS + g) for g in range(GROUPS)]))
        wide = top if before is None else jnp.concatenate([top] * (scores.shape[-1] // DH), axis=-1)
        weights = jnp.exp2((scores - wide) * RATE)
        rounded = weights.astype(jnp.bfloat16).reshape(GROUPS * rows, -1)
        value = values(head)
        few = value.shape[0] <= FEW
        if not few:
            value = jnp.concatenate([value, jnp.ones_like(value)], axis=1)
        mixed = lax.dot_general(rounded, value, (((1,), (0,)), ((), ())), preferred_element_type=jnp.float32)
        mixed = mixed.reshape(GROUPS, rows, -1)
        totals = jnp.sum(weights, axis=-1, keepdims=True) if few else mixed[:, :, DH:]
        for g in range(GROUPS):
            emit(head * GROUPS + g, mixed[g, :, :DH], totals[g], top[g])


def columns(h):
    return slice(h * DH, (h + 1) * DH)


def heads_of(ref, rows=slice(None), at=0):
    return lambda head: ref[rows, at + head * DH : at + (head + 1) * DH]


def pairs_of(ref, rows=slice(None)):
    def pair(head):
        both = ref[rows, head * WIDTH : (head + 1) * WIDTH]
        return jnp.concatenate([both[:, :DH], both[:, DH:]], axis=0)

    return pair


def in_parts(table):
    rest = jnp.where(lax.broadcasted_iota(jnp.int32, table.shape, 1) < HQ, table, 0.0)
    parts = jnp.zeros_like(table)
    for part in range(PARTS):
        piece = rest.astype(jnp.bfloat16).astype(jnp.float32)
        parts = parts + (pltpu.roll(piece, part * HQ, 1) if part else piece)
        rest = rest - piece
    return parts.astype(jnp.bfloat16)


def own_kernel(
    first_ref, len_ref, q_ref, k_ref, v_ref, acc_ref, level_ref, start_ref, out_ref, mark_ref, ends_ref
):
    block = pl.program_id(0)

    @pl.when(block == 0)
    def _():
        ends_ref[...] = document_ends(len_ref[...])

    ends = ends_ref[...]
    first = first_ref[0].astype(jnp.float32)
    row = float_iota((BQ, 1), 0) + (block * BQ).astype(jnp.float32)
    start = jnp.max(jnp.where(ends <= row + first, ends, 0.0), axis=1, keepdims=True)
    mark_ref[block] = jnp.min(start)
    start_ref[...] = jnp.broadcast_to(start, start_ref.shape)

    def over(count):
        col = float_iota((BQ, count), 1)
        bias = jnp.where((col >= start - first) & (col <= row), 0.0, HIDDEN)

        def emit(h, mixed, total, top):
            mixed = mixed * (1.0 / total)
            acc_ref[:, columns(h)] = mixed
            out_ref[:, columns(h)] = mixed.astype(out_ref.dtype)
            level_ref[:, columns(h)] = jnp.broadcast_to(top + jnp.log2(total) * (1.0 / RATE), (BQ, DH))

        part = slice(0, count)
        attend(pairs_of(q_ref), heads_of(k_ref, part), heads_of(v_ref, part), bias, emit)

    for step in range(k_ref.shape[0] // BQ):
        pl.when(block == step)(functools.partial(over, (step + 1) * BQ))


def back_kernel(first_ref, len_ref, q_ref, k_ref, v_ref, slot_ref):
    first = first_ref[0]
    here = first.astype(jnp.float32)
    keys = k_ref.shape[0]
    block = pl.program_id(0)

    @pl.when((first // keys) % 2 == 0)
    def _():
        ends = document_ends(len_ref[...])
        edge = here + 2 * keys
        start = jnp.max(jnp.where(ends <= edge, ends, 0.0))
        right = jnp.min(jnp.where(ends > edge, ends, edge + edge)) - edge
        reached = start < here + keys
        by_keys = right > SLOT

        @pl.when(reached & by_keys)
        def _():
            rows = pl.ds(keys - SLOT + block * BQ, BQ)
            slot_ref[:, :KV] = k_ref[rows, :]
            slot_ref[:, KV : 2 * KV] = v_ref[rows, :]

        def over(count):
            row = float_iota((BQ, 1), 0) + (block * BQ).astype(jnp.float32)
            col = float_iota((BQ, count), 1)
            bias = jnp.where((col >= start - (here + keys - count)) & (row < right), 0.0, HIDDEN)
            lane = lax.broadcasted_iota(jnp.int32, (BQ, 128), 1)
            level = [jnp.zeros((BQ, 128), jnp.float32)]

            def emit(h, mixed, total, top):
                slot_ref[:, columns(h)] = (mixed * (1.0 / total)).astype(jnp.bfloat16)
                level[0] = jnp.where(lane == h, top * RATE + jnp.log2(total), level[0])

            part = slice(keys - count, keys)
            attend(pairs_of(q_ref), heads_of(k_ref, part), heads_of(v_ref, part), bias, emit)
            slot_ref[:, 2 * KV :] = in_parts(level[0])

        working = reached & jnp.logical_not(by_keys) & ((block * BQ).astype(jnp.float32) < right)
        length = here + keys - start
        pl.when(working & (length <= 256))(functools.partial(over, 256))
        pl.when(working & (length > 256) & (length <= 384))(functools.partial(over, 384))
        pl.when(working & (length > 384))(functools.partial(over, keys))


def rows_at(block):
    return pl.ds(pl.multiple_of(block * BQ, BQ), BQ)


def writer(done_ref, out_ref, sem):
    def copy(block):
        return pltpu.make_async_copy(done_ref.at[rows_at(block), :], out_ref.at[rows_at(block), :], sem.at[block])

    return copy


def added(rows, acc_ref, level_ref, write):
    def emit(h, mixed, total, top):
        keep = jnp.exp2((level_ref[rows, columns(h)] - top) * RATE)
        total = total + keep
        mixed = (mixed + keep * acc_ref[rows, columns(h)]) * (1.0 / total)
        write(h, mixed, lambda: top + jnp.log2(total) * (1.0 / RATE))

    return emit


def levels_of(level_ref, rows):
    return lambda h: level_ref[rows, columns(h)]


def next_kernel(
    first_ref, mark_ref, q_ref, k_ref, v_ref, acc_ref, level_ref, start_ref, prior_ref, out_ref, new_acc_ref,
    new_level_ref, done_ref, sem,
):
    keys = k_ref.shape[0]
    first = first_ref[0].astype(jnp.float32)
    base = first - keys
    blocks = q_ref.shape[0] // BQ
    copy = writer(done_ref, out_ref, sem)

    def finishes(block):
        return (mark_ref[block] < first) & (mark_ref[block] >= base)

    @pl.loop(0, blocks)
    def _(block):
        @pl.when(mark_ref[block] < first)
        def _():
            rows = rows_at(block)
            bias = jnp.where(float_iota((BQ, keys), 1) >= start_ref[rows, :1] - base, 0.0, HIDDEN)

            def write(h, mixed, level):
                new_acc_ref[rows, columns(h)] = mixed
                done_ref[rows, columns(h)] = mixed.astype(done_ref.dtype)
                new_level_ref[rows, columns(h)] = level()

            emit = added(rows, acc_ref, level_ref, write)
            attend(
                pairs_of(q_ref, rows), heads_of(k_ref), heads_of(v_ref), bias, emit, levels_of(level_ref, rows)
            )

        pl.when(finishes(block))(lambda: copy(block).start())

    @pl.loop(0, blocks)
    def _(block):
        pl.when(finishes(block))(lambda: copy(block).wait())


def last_kernel(
    first_ref, mark_ref, q_ref, slot_ref, k_ref, v_ref, acc_ref, level_ref, start_ref, prior_ref, out_ref,
    done_ref, sem,
):
    keys = k_ref.shape[0]
    first = first_ref[0].astype(jnp.float32)
    odd = (first_ref[0] // keys) % 2 == 1
    even = jnp.logical_not(odd)
    base = first - keys
    blocks = q_ref.shape[0] // BQ
    start = mark_ref[0]
    by_keys = mark_ref[SLOT // BQ] < first
    copy = writer(done_ref, out_ref, sem)

    def merge(block, ref_k, ref_v, at, count):
        rows = rows_at(block)
        skip = ref_k.shape[0] - count
        part = slice(skip, skip + count)
        bias = jnp.where(float_iota((BQ, count), 1) >= start_ref[rows, :1] - (base - count), 0.0, HIDDEN)

        def write(h, mixed, level):
            done_ref[rows, columns(h)] = mixed.astype(done_ref.dtype)

        emit = added(rows, acc_ref, level_ref, write)
        attend(
            pairs_of(q_ref, rows), heads_of(ref_k, part), heads_of(ref_v, part, at), bias, emit,
            levels_of(level_ref, rows),
        )

    def combine(block):
        rows = rows_at(block)
        parts = slot_ref[rows, 2 * KV :].astype(jnp.float32)
        there = parts
        for part in range(1, PARTS):
            there = there + pltpu.roll(parts, 128 - part * HQ, 1)
        for h in range(HQ):
            here = level_ref[rows, columns(h)] * RATE
            other = jnp.broadcast_to(there[:, h : h + 1], here.shape)
            top = jnp.maximum(here, other)
            keep, take = jnp.exp2(here - top), jnp.exp2(other - top)
            mixed = keep * acc_ref[rows, columns(h)] + take * slot_ref[rows, columns(h)].astype(jnp.float32)
            done_ref[rows, columns(h)] = (mixed * (1.0 / (keep + take))).astype(done_ref.dtype)

    def sweep(condition, work, end=blocks):
        @pl.when(condition & (start < base))
        def _():
            @pl.loop(0, end)
            def _(block):
                @pl.when(mark_ref[block] < base)
                def _():
                    work(block)
                    copy(block).start()

    near = start >= base - BQ
    far = start < base - SLOT
    some = jnp.logical_not(near | far)
    sweep(odd & near, lambda block: merge(block, k_ref, v_ref, 0, BQ))
    sweep(odd & some, lambda block: merge(block, k_ref, v_ref, 0, SLOT))
    sweep(odd & far, lambda block: merge(block, k_ref, v_ref, 0, keys))
    sweep(even & by_keys & near, lambda block: merge(block, slot_ref, slot_ref, KV, BQ))
    sweep(even & by_keys & jnp.logical_not(near), lambda block: merge(block, slot_ref, slot_ref, KV, SLOT))
    sweep(even & jnp.logical_not(by_keys), combine, SLOT // BQ)

    @pl.loop(0, blocks)
    def _(block):
        pl.when(mark_ref[block] < base)(lambda: copy(block).wait())


def rows_of(width):
    return pl.BlockSpec((BQ, width), lambda i: (i, 0))


SMEM = pl.BlockSpec(memory_space=pltpu.SMEM)
WHOLE = pl.BlockSpec(memory_space=pltpu.VMEM)
ANY = pl.BlockSpec(memory_space=pl.ANY)
WIDE = HQ * DH


def cost(rows, keys):
    return pl.CostEstimate(
        flops=4 * rows * keys * WIDE, bytes_accessed=rows * WIDE * 8, transcendentals=rows * keys * HQ
    )


PARAMS = pltpu.CompilerParams(vmem_limit_bytes=VMEM)


def f32(*shape):
    return jax.ShapeDtypeStruct(shape, jnp.float32)


def bf16(*shape):
    return jax.ShapeDtypeStruct(shape, jnp.bfloat16)


def own_stage(first, lengths, queries, keys, values):
    rows = queries.shape[0]
    return pl.pallas_call(
        own_kernel,
        grid=(rows // BQ,),
        in_specs=[SMEM, WHOLE, rows_of(WIDE), WHOLE, WHOLE],
        out_specs=[rows_of(WIDE), rows_of(WIDE), rows_of(128), rows_of(WIDE), SMEM],
        out_shape=[f32(rows, WIDE), f32(rows, WIDE), f32(rows, 128), bf16(rows, WIDE), f32(rows // BQ)],
        scratch_shapes=[pltpu.VMEM(lengths.shape, jnp.float32)],
        cost_estimate=cost(rows, keys.shape[0]),
        compiler_params=PARAMS,
        name="own_shard",
        interpret=INTERPRET,
    )(first, lengths, queries, keys, values)


def copy_kernel(in_ref, out_ref, sem):
    copy = pltpu.make_async_copy(in_ref.at[pl.ds(0, out_ref.shape[0]), :], out_ref, sem)
    copy.start()
    copy.wait()


def leading_rows(array, rows):
    return pl.pallas_call(
        copy_kernel,
        in_specs=[pl.BlockSpec(memory_space=pltpu.HBM)],
        out_specs=WHOLE,
        out_shape=jax.ShapeDtypeStruct((rows, array.shape[1]), array.dtype),
        scratch_shapes=[pltpu.SemaphoreType.DMA],
        compiler_params=PARAMS,
        name="leading_rows",
        interpret=INTERPRET,
    )(pltpu.with_memory_space_constraint(array, pltpu.HBM))


def back_stage(first, lengths, queries, keys, values):
    return pl.pallas_call(
        back_kernel,
        grid=(SLOT // BQ,),
        in_specs=[SMEM, WHOLE, rows_of(WIDE), WHOLE, WHOLE],
        out_specs=rows_of(2 * KV + 128),
        out_shape=bf16(SLOT, 2 * KV + 128),
        cost_estimate=cost(SLOT, keys.shape[0]),
        compiler_params=PARAMS,
        name="back_shard",
        interpret=INTERPRET,
    )(first, lengths, queries, keys, values)


def writing(rows):
    return [
        pltpu.VMEM((rows, WIDE), jnp.bfloat16),
        pltpu.SemaphoreType.DMA((rows // BQ,)),
    ]


def next_stage(first, marks, queries, keys, values, acc, levels, starts, prior):
    rows = queries.shape[0]
    return pl.pallas_call(
        next_kernel,
        in_specs=[SMEM] * 2 + [WHOLE] * 6 + [ANY],
        out_specs=[ANY, WHOLE, WHOLE],
        out_shape=[bf16(rows, WIDE), f32(rows, WIDE), f32(rows, WIDE)],
        scratch_shapes=writing(rows),
        input_output_aliases={8: 0},
        cost_estimate=cost(rows, keys.shape[0]),
        compiler_params=PARAMS,
        name="next_shard",
        interpret=INTERPRET,
    )(first, marks, queries, keys, values, acc, levels, starts, prior)


def last_stage(first, marks, queries, slot, keys, values, acc, levels, starts, prior):
    rows = queries.shape[0]
    return pl.pallas_call(
        last_kernel,
        in_specs=[SMEM] * 2 + [WHOLE] * 7 + [ANY],
        out_specs=ANY,
        out_shape=bf16(rows, WIDE),
        scratch_shapes=writing(rows),
        input_output_aliases={9: 0},
        cost_estimate=cost(rows, SLOT),
        compiler_params=PARAMS,
        name="last_shard",
        interpret=INTERPRET,
    )(first, marks, queries, slot, keys, values, acc, levels, starts, prior)


def on_device(queries, keys, values, doc_lengths):
    count = lax.axis_size("cp")
    first = (lax.axis_index("cp").astype(jnp.int32) * queries.shape[0]).reshape(1)
    lengths = doc_lengths.reshape(1, -1)
    evens = range(0, count, 2)

    def hop(array, pairs):
        return lax.ppermute(array, "cp", pairs)

    onward = [(i, i + 1) for i in range(count - 1)]
    one_k = hop(keys, onward)
    one_v = hop(values, onward)
    guests = hop(leading_rows(queries, SLOT), [(i, i - 2) for i in evens if i])
    acc, levels, starts, out, marks = own_stage(first, lengths, queries, keys, values)
    slot = back_stage(first, lengths, guests, keys, values)
    slot = hop(slot, [(i, i + 2) for i in evens if i + 2 < count])
    across = [(i, i + 1) for i in evens]
    two_k = hop(one_k, across)
    two_v = hop(one_v, across)
    out, acc, levels = next_stage(first, marks, queries, one_k, one_v, acc, levels, starts, out)
    out = last_stage(first, marks, queries, slot, two_k, two_v, acc, levels, starts, out)
    return out


def solution(mesh):
    return jax.shard_map(
        on_device,
        mesh=mesh,
        in_specs=(P(("grp", "cp"), None), P(("grp", "cp"), None), P(("grp", "cp"), None), P("grp")),
        out_specs=P(("grp", "cp"), None),
        check_vma=False,
    )
```

```python
import functools
import math

import jax
import jax.numpy as jnp
from jax import lax
from jax.experimental import pallas as pl
from jax.experimental.pallas import tpu as pltpu
from jax.sharding import PartitionSpec as P


HQ = 16
HK = 8
DH = 128
GROUPS = HQ // HK
WIDTH = GROUPS * DH
KV = HK * DH
BQ = 128
HIDDEN = -1e30
RATE = math.log2(math.e) * 144.0 ** -0.5
PARTS = 3
VMEM = 16 << 20
FEW = 128
INTERPRET = False

SLOT = 256


def document_ends(lengths):
    docs = lengths.shape[1]
    sub = lax.broadcasted_iota(jnp.int32, (docs, docs), 0)
    lane = lax.broadcasted_iota(jnp.int32, (docs, docs), 1)
    rows = jnp.broadcast_to(lengths.astype(jnp.float32), (docs, docs))
    column = jnp.sum(jnp.where(sub == lane, rows, 0.0), axis=1, keepdims=True)
    return jnp.sum(jnp.where(sub <= lane, column, 0.0), axis=0, keepdims=True)


def float_iota(shape, axis):
    return lax.broadcasted_iota(jnp.int32, shape, axis).astype(jnp.float32)


def attend(pair, keys, values, bias, emit, before=None):
    rows = bias.shape[0]

    def score(head):
        return lax.dot_general(pair(head), keys(head), (((1,), (1,)), ((), ())), preferred_element_type=jnp.float32)

    ahead = score(0)
    for head in range(HK):
        scores = ahead
        if head + 1 < HK:
            ahead = score(head + 1)
        scores = scores.reshape(GROUPS, rows, -1) + bias[None]
        top = jnp.max(scores, axis=-1, keepdims=True)
        if before is not None:
            top = jnp.maximum(top, jnp.stack([before(head * GROUPS + g) for g in range(GROUPS)]))
        wide = top if before is None else jnp.concatenate([top] * (scores.shape[-1] // DH), axis=-1)
        weights = jnp.exp2((scores - wide) * RATE)
        rounded = weights.astype(jnp.bfloat16).reshape(GROUPS * rows, -1)
        value = values(head)
        few = value.shape[0] <= FEW
        if not few:
            value = jnp.concatenate([value, jnp.ones_like(value)], axis=1)
        mixed = lax.dot_general(rounded, value, (((1,), (0,)), ((), ())), preferred_element_type=jnp.float32)
        mixed = mixed.reshape(GROUPS, rows, -1)
        totals = jnp.sum(weights, axis=-1, keepdims=True) if few else mixed[:, :, DH:]
        for g in range(GROUPS):
            emit(head * GROUPS + g, mixed[g, :, :DH], totals[g], top[g])


def columns(h):
    return slice(h * DH, (h + 1) * DH)


def heads_of(ref, rows=slice(None), at=0):
    return lambda head: ref[rows, at + head * DH : at + (head + 1) * DH]


def pairs_of(ref, rows=slice(None)):
    def pair(head):
        both = ref[rows, head * WIDTH : (head + 1) * WIDTH]
        return jnp.concatenate([both[:, :DH], both[:, DH:]], axis=0)

    return pair


def in_parts(table):
    rest = jnp.where(lax.broadcasted_iota(jnp.int32, table.shape, 1) < HQ, table, 0.0)
    parts = jnp.zeros_like(table)
    for part in range(PARTS):
        piece = rest.astype(jnp.bfloat16).astype(jnp.float32)
        parts = parts + (pltpu.roll(piece, part * HQ, 1) if part else piece)
        rest = rest - piece
    return parts.astype(jnp.bfloat16)


def own_kernel(
    first_ref, len_ref, q_ref, k_ref, v_ref, acc_ref, level_ref, start_ref, out_ref, mark_ref, ends_ref
):
    block = pl.program_id(0)

    @pl.when(block == 0)
    def _():
        ends_ref[...] = document_ends(len_ref[...])

    ends = ends_ref[...]
    first = first_ref[0].astype(jnp.float32)
    row = float_iota((BQ, 1), 0) + (block * BQ).astype(jnp.float32)
    start = jnp.max(jnp.where(ends <= row + first, ends, 0.0), axis=1, keepdims=True)
    mark_ref[block] = jnp.min(start)
    start_ref[...] = jnp.broadcast_to(start, start_ref.shape)

    def over(count):
        col = float_iota((BQ, count), 1)
        bias = jnp.where((col >= start - first) & (col <= row), 0.0, HIDDEN)

        def emit(h, mixed, total, top):
            mixed = mixed * (1.0 / total)
            acc_ref[:, columns(h)] = mixed
            out_ref[:, columns(h)] = mixed.astype(out_ref.dtype)
            level_ref[:, columns(h)] = jnp.broadcast_to(top + jnp.log2(total) * (1.0 / RATE), (BQ, DH))

        part = slice(0, count)
        attend(pairs_of(q_ref), heads_of(k_ref, part), heads_of(v_ref, part), bias, emit)

    for step in range(k_ref.shape[0] // BQ):
        pl.when(block == step)(functools.partial(over, (step + 1) * BQ))


def back_kernel(first_ref, len_ref, q_ref, k_ref, v_ref, slot_ref):
    first = first_ref[0]
    here = first.astype(jnp.float32)
    keys = k_ref.shape[0]
    block = pl.program_id(0)

    @pl.when((first // keys) % 2 == 0)
    def _():
        ends = document_ends(len_ref[...])
        edge = here + 2 * keys
        start = jnp.max(jnp.where(ends <= edge, ends, 0.0))
        right = jnp.min(jnp.where(ends > edge, ends, edge + edge)) - edge
        reached = start < here + keys
        by_keys = here + keys - start <= SLOT

        @pl.when(reached & by_keys)
        def _():
            rows = pl.ds(keys - SLOT + block * BQ, BQ)
            slot_ref[:, :KV] = k_ref[rows, :]
            slot_ref[:, KV : 2 * KV] = v_ref[rows, :]

        def over(count):
            row = float_iota((BQ, 1), 0) + (block * BQ).astype(jnp.float32)
            col = float_iota((BQ, count), 1)
            bias = jnp.where((col >= start - (here + keys - count)) & (row < right), 0.0, HIDDEN)
            lane = lax.broadcasted_iota(jnp.int32, (BQ, 128), 1)
            level = [jnp.zeros((BQ, 128), jnp.float32)]

            def emit(h, mixed, total, top):
                slot_ref[:, columns(h)] = (mixed * (1.0 / total)).astype(jnp.bfloat16)
                level[0] = jnp.where(lane == h, top * RATE + jnp.log2(total), level[0])

            part = slice(keys - count, keys)
            attend(pairs_of(q_ref), heads_of(k_ref, part), heads_of(v_ref, part), bias, emit)
            slot_ref[:, 2 * KV :] = in_parts(level[0])

        working = reached & jnp.logical_not(by_keys) & ((block * BQ).astype(jnp.float32) < right)
        length = here + keys - start
        pl.when(working & (length <= 384))(functools.partial(over, 384))
        pl.when(working & (length > 384))(functools.partial(over, keys))


def rows_at(block):
    return pl.ds(pl.multiple_of(block * BQ, BQ), BQ)


def writer(done_ref, out_ref, sem):
    def copy(block):
        return pltpu.make_async_copy(done_ref.at[rows_at(block), :], out_ref.at[rows_at(block), :], sem.at[block])

    return copy


def added(rows, acc_ref, level_ref, write):
    def emit(h, mixed, total, top):
        keep = jnp.exp2((level_ref[rows, columns(h)] - top) * RATE)
        total = total + keep
        mixed = (mixed + keep * acc_ref[rows, columns(h)]) * (1.0 / total)
        write(h, mixed, lambda: top + jnp.log2(total) * (1.0 / RATE))

    return emit


def levels_of(level_ref, rows):
    return lambda h: level_ref[rows, columns(h)]


def next_kernel(
    first_ref, mark_ref, q_ref, k_ref, v_ref, acc_ref, level_ref, start_ref, prior_ref, out_ref, new_acc_ref,
    new_level_ref, done_ref, sem,
):
    keys = k_ref.shape[0]
    first = first_ref[0].astype(jnp.float32)
    base = first - keys
    blocks = q_ref.shape[0] // BQ
    copy = writer(done_ref, out_ref, sem)

    def finishes(block):
        return (mark_ref[block] < first) & (mark_ref[block] >= base)

    @pl.loop(0, blocks)
    def _(block):
        @pl.when(mark_ref[block] < first)
        def _():
            rows = rows_at(block)
            bias = jnp.where(float_iota((BQ, keys), 1) >= start_ref[rows, :1] - base, 0.0, HIDDEN)

            def write(h, mixed, level):
                new_acc_ref[rows, columns(h)] = mixed
                done_ref[rows, columns(h)] = mixed.astype(done_ref.dtype)
                new_level_ref[rows, columns(h)] = level()

            emit = added(rows, acc_ref, level_ref, write)
            attend(
                pairs_of(q_ref, rows), heads_of(k_ref), heads_of(v_ref), bias, emit, levels_of(level_ref, rows)
            )

        pl.when(finishes(block))(lambda: copy(block).start())

    @pl.loop(0, blocks)
    def _(block):
        pl.when(finishes(block))(lambda: copy(block).wait())


def last_kernel(
    first_ref, mark_ref, q_ref, slot_ref, k_ref, v_ref, acc_ref, level_ref, start_ref, prior_ref, out_ref,
    done_ref, sem,
):
    keys = k_ref.shape[0]
    first = first_ref[0].astype(jnp.float32)
    odd = (first_ref[0] // keys) % 2 == 1
    even = jnp.logical_not(odd)
    base = first - keys
    blocks = q_ref.shape[0] // BQ
    start = mark_ref[0]
    by_keys = base - start <= SLOT
    copy = writer(done_ref, out_ref, sem)

    def merge(block, ref_k, ref_v, at, count):
        rows = rows_at(block)
        skip = ref_k.shape[0] - count
        part = slice(skip, skip + count)
        bias = jnp.where(float_iota((BQ, count), 1) >= start_ref[rows, :1] - (base - count), 0.0, HIDDEN)

        def write(h, mixed, level):
            done_ref[rows, columns(h)] = mixed.astype(done_ref.dtype)

        emit = added(rows, acc_ref, level_ref, write)
        attend(
            pairs_of(q_ref, rows), heads_of(ref_k, part), heads_of(ref_v, part, at), bias, emit,
            levels_of(level_ref, rows),
        )

    def combine(block):
        rows = rows_at(block)
        parts = slot_ref[rows, 2 * KV :].astype(jnp.float32)
        there = parts
        for part in range(1, PARTS):
            there = there + pltpu.roll(parts, 128 - part * HQ, 1)
        for h in range(HQ):
            here = level_ref[rows, columns(h)] * RATE
            other = jnp.broadcast_to(there[:, h : h + 1], here.shape)
            top = jnp.maximum(here, other)
            keep, take = jnp.exp2(here - top), jnp.exp2(other - top)
            mixed = keep * acc_ref[rows, columns(h)] + take * slot_ref[rows, columns(h)].astype(jnp.float32)
            done_ref[rows, columns(h)] = (mixed * (1.0 / (keep + take))).astype(done_ref.dtype)

    def sweep(condition, work, end=blocks):
        @pl.when(condition & (start < base))
        def _():
            @pl.loop(0, end)
            def _(block):
                @pl.when(mark_ref[block] < base)
                def _():
                    work(block)
                    copy(block).start()

    near = start >= base - BQ
    far = start < base - SLOT
    some = jnp.logical_not(near | far)
    sweep(odd & near, lambda block: merge(block, k_ref, v_ref, 0, BQ))
    sweep(odd & some, lambda block: merge(block, k_ref, v_ref, 0, SLOT))
    sweep(odd & far, lambda block: merge(block, k_ref, v_ref, 0, keys))
    sweep(even & by_keys & near, lambda block: merge(block, slot_ref, slot_ref, KV, BQ))
    sweep(even & by_keys & jnp.logical_not(near), lambda block: merge(block, slot_ref, slot_ref, KV, SLOT))
    sweep(even & jnp.logical_not(by_keys), combine, SLOT // BQ)

    @pl.loop(0, blocks)
    def _(block):
        pl.when(mark_ref[block] < base)(lambda: copy(block).wait())


def rows_of(width):
    return pl.BlockSpec((BQ, width), lambda i: (i, 0))


SMEM = pl.BlockSpec(memory_space=pltpu.SMEM)
WHOLE = pl.BlockSpec(memory_space=pltpu.VMEM)
ANY = pl.BlockSpec(memory_space=pl.ANY)
WIDE = HQ * DH


def cost(rows, keys):
    return pl.CostEstimate(
        flops=4 * rows * keys * WIDE, bytes_accessed=rows * WIDE * 8, transcendentals=rows * keys * HQ
    )


PARAMS = pltpu.CompilerParams(vmem_limit_bytes=VMEM)


def f32(*shape):
    return jax.ShapeDtypeStruct(shape, jnp.float32)


def bf16(*shape):
    return jax.ShapeDtypeStruct(shape, jnp.bfloat16)


def own_stage(first, lengths, queries, keys, values):
    rows = queries.shape[0]
    return pl.pallas_call(
        own_kernel,
        grid=(rows // BQ,),
        in_specs=[SMEM, WHOLE, rows_of(WIDE), WHOLE, WHOLE],
        out_specs=[rows_of(WIDE), rows_of(WIDE), rows_of(128), rows_of(WIDE), SMEM],
        out_shape=[f32(rows, WIDE), f32(rows, WIDE), f32(rows, 128), bf16(rows, WIDE), f32(rows // BQ)],
        scratch_shapes=[pltpu.VMEM(lengths.shape, jnp.float32)],
        cost_estimate=cost(rows, keys.shape[0]),
        compiler_params=PARAMS,
        name="own_shard",
        interpret=INTERPRET,
    )(first, lengths, queries, keys, values)


def copy_kernel(in_ref, out_ref, sem):
    copy = pltpu.make_async_copy(in_ref.at[pl.ds(0, out_ref.shape[0]), :], out_ref, sem)
    copy.start()
    copy.wait()


def leading_rows(array, rows):
    return pl.pallas_call(
        copy_kernel,
        in_specs=[pl.BlockSpec(memory_space=pltpu.HBM)],
        out_specs=WHOLE,
        out_shape=jax.ShapeDtypeStruct((rows, array.shape[1]), array.dtype),
        scratch_shapes=[pltpu.SemaphoreType.DMA],
        compiler_params=PARAMS,
        name="leading_rows",
        interpret=INTERPRET,
    )(pltpu.with_memory_space_constraint(array, pltpu.HBM))


def back_stage(first, lengths, queries, keys, values):
    return pl.pallas_call(
        back_kernel,
        grid=(SLOT // BQ,),
        in_specs=[SMEM, WHOLE, rows_of(WIDE), WHOLE, WHOLE],
        out_specs=rows_of(2 * KV + 128),
        out_shape=bf16(SLOT, 2 * KV + 128),
        cost_estimate=cost(SLOT, keys.shape[0]),
        compiler_params=PARAMS,
        name="back_shard",
        interpret=INTERPRET,
    )(first, lengths, queries, keys, values)


def writing(rows):
    return [
        pltpu.VMEM((rows, WIDE), jnp.bfloat16),
        pltpu.SemaphoreType.DMA((rows // BQ,)),
    ]


def next_stage(first, marks, queries, keys, values, acc, levels, starts, prior):
    rows = queries.shape[0]
    return pl.pallas_call(
        next_kernel,
        in_specs=[SMEM] * 2 + [WHOLE] * 6 + [ANY],
        out_specs=[ANY, WHOLE, WHOLE],
        out_shape=[bf16(rows, WIDE), f32(rows, WIDE), f32(rows, WIDE)],
        scratch_shapes=writing(rows),
        input_output_aliases={8: 0},
        cost_estimate=cost(rows, keys.shape[0]),
        compiler_params=PARAMS,
        name="next_shard",
        interpret=INTERPRET,
    )(first, marks, queries, keys, values, acc, levels, starts, prior)


def last_stage(first, marks, queries, slot, keys, values, acc, levels, starts, prior):
    rows = queries.shape[0]
    return pl.pallas_call(
        last_kernel,
        in_specs=[SMEM] * 2 + [WHOLE] * 7 + [ANY],
        out_specs=ANY,
        out_shape=bf16(rows, WIDE),
        scratch_shapes=writing(rows),
        input_output_aliases={9: 0},
        cost_estimate=cost(rows, SLOT),
        compiler_params=PARAMS,
        name="last_shard",
        interpret=INTERPRET,
    )(first, marks, queries, slot, keys, values, acc, levels, starts, prior)


def on_device(queries, keys, values, doc_lengths):
    count = lax.axis_size("cp")
    first = (lax.axis_index("cp").astype(jnp.int32) * queries.shape[0]).reshape(1)
    lengths = doc_lengths.reshape(1, -1)
    evens = range(0, count, 2)

    def hop(array, pairs):
        return lax.ppermute(array, "cp", pairs)

    onward = [(i, i + 1) for i in range(count - 1)]
    one_k = hop(keys, onward)
    one_v = hop(values, onward)
    guests = hop(leading_rows(queries, SLOT), [(i, i - 2) for i in evens if i])
    acc, levels, starts, out, marks = own_stage(first, lengths, queries, keys, values)
    slot = back_stage(first, lengths, guests, keys, values)
    slot = hop(slot, [(i, i + 2) for i in evens if i + 2 < count])
    across = [(i, i + 1) for i in evens]
    two_k = hop(one_k, across)
    two_v = hop(one_v, across)
    out, acc, levels = next_stage(first, marks, queries, one_k, one_v, acc, levels, starts, out)
    out = last_stage(first, marks, queries, slot, two_k, two_v, acc, levels, starts, out)
    return out


def solution(mesh):
    return jax.shard_map(
        on_device,
        mesh=mesh,
        in_specs=(P(("grp", "cp"), None), P(("grp", "cp"), None), P(("grp", "cp"), None), P("grp")),
        out_specs=P(("grp", "cp"), None),
        check_vma=False,
    )
```
